512 devices in a mesh: panel: 32 (over y_lo, z, core), rhs: 16 (over x, y_hi).
Axes of the slice: x: 4, y: 8 (y_hi: 4, y_lo: 2; y = y_hi * 2 + y_lo), z: 8, core: 2. Of those that a mesh axis runs over, the one named last changes fastest.
Arguments:
- pivot_rhs: float32 [2, 2048, 2048], P(None, 'panel', 'rhs'), may hold values from -6 to 6
- update_rhs: float32 [4096, 2048], P('panel', 'rhs'), may hold values from -6 to 6
- parent_rhs: float32 [4096, 2048], P('panel', 'rhs'), may hold values from -6 to 6
- lower_pivot: bfloat16 [2, 2048, 2048], P(None, 'panel', 'rhs'), may hold values from -1 to 1.4, as said below
- lower_update: bfloat16 [4096, 2048], P('panel', 'rhs'), may hold values from -0.125 to 0.125
- parent_lower: bfloat16 [4096, 4096], P('panel', 'rhs'), may hold values from -1 to 1.4, as said below
- parent_upper: bfloat16 [4096, 4096], P('panel', 'rhs'), may hold values from -1 to 1.4, as said below
- upper_pivot: bfloat16 [2, 2048, 2048], P(None, 'panel', 'rhs'), may hold values from -1 to 1.4, as said below
- upper_update: bfloat16 [2, 2048, 2048], P(None, 'panel', 'rhs'), may hold values from -0.125 to 0.125
- maps: int32 [4096], replicated, may hold values from 0 to 4095, as said below
Outputs:
- parent_solution: float32 [4096, 2048], P('panel', 'rhs')
- child_solution: float32 [2, 2048, 2048], P(None, 'panel', 'rhs')
The draws below stay inside these ranges and needn't reach their ends.
Inputs may be any that keep to these rules, and one draw needn't show every extreme that they name: `maps`: for each child k, entry k * 2048 + i is 2 * i + b with b equal to 0 or 1; both values of b occur for each child in every draw. `lower_pivot`: each block is lower triangular, diagonal 0.6 to 1.4. `upper_pivot`: each block is upper triangular, diagonal 0.6 to 1.4. `parent_lower`: lower triangular, diagonal 0.6 to 1.4. `parent_upper`: upper triangular, diagonal 0.6 to 1.4.
All inputs are finite; a program needn't handle non-finite values.
Results may differ from the reference program's by a relative error of at most 0.0054.
Values may be sent and summed in bfloat16 or wider, within the bound.
A program may use at most 64 MiB of HBM per device.

```python
import math
import jax
import jax.numpy as jnp
from jax import lax

F = 4096
KC = 2048
FU = 2048
RHS = 2048


def triangle(random_key, block_count, matrix_order, lower_side):
    shape_full = (block_count, matrix_order, matrix_order)
    noise = jax.random.normal(random_key, shape_full, jnp.float32)
    noise = noise / math.sqrt(matrix_order)
    row_ids = lax.broadcasted_iota(jnp.int32, (matrix_order, matrix_order), 0)
    col_ids = lax.broadcasted_iota(jnp.int32, (matrix_order, matrix_order), 1)
    if lower_side:
        keeper = row_ids > col_ids
    else:
        keeper = row_ids < col_ids
    diagonal_scale = jax.random.uniform(jax.random.fold_in(random_key, 7), (block_count, matrix_order, 1), jnp.float32, 0.6, 1.4)
    identity = jnp.where(row_ids == col_ids, 1.0, 0.0).astype(jnp.float32)
    return jnp.where(keeper[None], noise, 0.0) + identity[None] * diagonal_scale


def draw_lower_pivot(key, part):
    return triangle(jax.random.fold_in(key, 101), 2, KC, True).astype(jnp.bfloat16)


def draw_upper_pivot(key, part):
    return triangle(jax.random.fold_in(key, 103), 2, KC, False).astype(jnp.bfloat16)


def draw_parent_lower(key, part):
    return triangle(jax.random.fold_in(key, 107), 1, F, True).reshape(F, F).astype(jnp.bfloat16)


def draw_parent_upper(key, part):
    return triangle(jax.random.fold_in(key, 109), 1, F, False).reshape(F, F).astype(jnp.bfloat16)


def draw_maps(key, part):
    local = lax.broadcasted_iota(jnp.int32, (FU,), 0)
    first_bits = jax.random.randint(jax.random.fold_in(key, 211), (FU,), 0, 2)
    first_bits = jnp.where(local == 0, 0, first_bits)
    first_bits = jnp.where(local == FU - 1, 1, first_bits)
    second_bits = jax.random.randint(jax.random.fold_in(key, 212), (FU,), 0, 2)
    second_bits = jnp.where(local == 0, 1, second_bits)
    second_bits = jnp.where(local == FU - 1, 0, second_bits)
    return jnp.concatenate([2 * local + first_bits, 2 * local + second_bits]).astype(jnp.int32)


def levels(key, dims, shards, smallest, top_value):
    factor_of, own = 1.0, jax.random.fold_in(key, 6)
    for axis_at, blocks in shards:
        draws = jnp.exp(jax.random.uniform(jax.random.fold_in(own, axis_at), (blocks,), jnp.float32, smallest / len(shards), top_value / len(shards)))
        factor_of = factor_of * jnp.repeat(draws, dims[axis_at] // blocks).reshape([-1 if axis == axis_at else 1 for axis in range(len(dims))])
    return factor_of


def normal_values(stream_key, extent, spread, bound, pieces=(), held_as=jnp.bfloat16):
    level = levels(stream_key, extent, pieces, -0.22, 0.18) if pieces else 1.0
    drawn = jax.random.normal(stream_key, extent, jnp.float32) * spread * level
    return jnp.minimum(jnp.maximum(drawn, -bound), bound).astype(held_as)


def setup_inputs(seed: int = 0) -> dict:
    key_of = jax.random.split(jax.random.key(seed), 11)
    return {
        "pivot_rhs": normal_values(key_of[0], (2, KC, RHS), 1.0, 6.0, ((1, 32), (2, 16)), jnp.float32),
        "update_rhs": normal_values(key_of[1], (2 * FU, RHS), 1.0, 6.0, ((0, 32), (1, 16)), jnp.float32),
        "parent_rhs": normal_values(key_of[2], (F, RHS), 1.0, 6.0, ((0, 32), (1, 16)), jnp.float32),
        "lower_pivot": draw_lower_pivot(jax.random.fold_in(key_of[10], 71), 0),
        "lower_update": normal_values(key_of[4], (2 * FU, KC), KC ** -0.5, 0.125, ((0, 32), (1, 16))),
        "parent_lower": draw_parent_lower(jax.random.fold_in(key_of[10], 71), 0),
        "parent_upper": draw_parent_upper(jax.random.fold_in(key_of[10], 71), 0),
        "upper_pivot": draw_upper_pivot(jax.random.fold_in(key_of[10], 71), 0),
        "upper_update": normal_values(key_of[8], (2, KC, FU), FU ** -0.5, 0.125, ((1, 32), (2, 16))),
        "maps": draw_maps(jax.random.fold_in(key_of[10], 71), 0),
    }


def product(left, right):
    return jnp.dot(left, right, preferred_element_type=jnp.float32)


def reference(pivot_rhs, update_rhs, parent_rhs, lower_pivot, lower_update, parent_lower, parent_upper, upper_pivot, upper_update, maps):
    pivot_input = pivot_rhs.astype(jnp.bfloat16)
    solved = []
    updates = []
    for member in range(2):
        source = pivot_input[member]
        solved.append(product(lower_pivot[member], source))
        updates.append(update_rhs[member * FU:(member + 1) * FU] + product(lower_update[member * FU:(member + 1) * FU], source))
    pivot_half = jnp.stack(solved, axis=0).astype(jnp.bfloat16)
    update_half = jnp.concatenate(updates, axis=0).astype(jnp.bfloat16)
    widened = lax.optimization_barrier(update_half).astype(jnp.float32)
    scattered = jnp.zeros(parent_rhs.shape, jnp.float32).at[maps].add(widened)
    parent_sum = parent_rhs + scattered
    parent_mid = product(parent_lower, parent_sum.astype(jnp.bfloat16))
    parent_solution = product(parent_upper, parent_mid.astype(jnp.bfloat16))
    solution_half = parent_solution.astype(jnp.bfloat16)
    blocks = []
    for member in range(2):
        picked = jnp.take(solution_half, maps[member * FU:(member + 1) * FU], axis=0)
        direct = product(upper_pivot[member], pivot_half[member])
        blocks.append(direct + product(upper_update[member], picked))
    return parent_solution, jnp.stack(blocks, axis=0)
```

```python
import jax
import jax.numpy as jnp
from jax import lax
from jax.experimental import pallas as pl
from jax.experimental.pallas import tpu as pltpu
from jax.sharding import PartitionSpec as P

MESH = pl.DeviceIdType.MESH
BF = jnp.bfloat16
F32 = jnp.float32
NZ = 8
NP = 32
NQ = 16
NT = (((1,), (1,)), ((), ()))
NN = (((1,), (0,)), ((), ()))

LU, LP, PLO, PUP, UP, UU = range(6)


def dot(a, b, dims):
    return lax.dot_general(a, b, dims, preferred_element_type=F32)


def body(
    pivot_ref, update_ref, parent_ref, lp_ref, lu_ref, pl_ref, pu_ref, up_ref, uu_ref, maps_ref,
    sol_ref, child_ref,
    v, fs, fl, lu_in, upd_in, lu_out,
    g_send, g_recv, f_send, f_recv, m_send, m_recv,
):
    p = lax.axis_index("panel")
    q = lax.axis_index("rhs")
    yl = p // 16
    z = lax.rem(p // 2, NZ)
    c = lax.rem(p, 2)
    t = p // 2
    x = q // 4
    yh = lax.rem(q, 4)

    def panel_of(yl_, z_, c_):
        return yl_ * 16 + z_ * 2 + c_

    def z_at(d):
        return lax.rem(z + d, NZ)

    def q_at(dx, dy):
        return lax.rem(x + dx, 4) * 4 + lax.rem(yh + dy, 4)

    def signal(dev, sem):
        pl.semaphore_signal(sem, inc=1, device_id=dev, device_id_type=MESH)

    def fblock(a, qq):
        if a == PLO:
            return fl.at[0, pl.ds(2 * qq, 2)]
        if a == PUP:
            return fl.at[1, pl.ds(2 * qq, 2)]
        return fs.at[{LU: 0, LP: 1, UP: 2, UU: 3}[a], pl.ds(2 * qq, 2)]

    def needed(a, qq):
        if a in (LP, PLO):
            return qq <= t
        if a in (PUP, UP):
            return qq >= t
        return None

    def when(cond, fn):
        if cond is None:
            fn()
        else:
            pl.when(cond)(fn)

    def fcopy(a, qq, dev, sidx):
        return pltpu.make_async_remote_copy(
            src_ref=fblock(a, qq), dst_ref=fblock(a, qq),
            send_sem=f_send.at[a, sidx], recv_sem=f_recv.at[a, qq],
            device_id=dev, device_id_type=MESH,
        )

    def y_phase(a):
        def go():
            for i, dy in enumerate((1, 3, 2)):
                fcopy(a, q, (p, q_at(0, dy)), i).start()
            for i, dx in enumerate((1, 3, 2)):
                fcopy(a, q, (p, q_at(dx, 0)), 3 + i).start()
        when(needed(a, q), go)

    def x_phase(a):
        for j, dy in enumerate((1, 3, 2)):
            qq = q_at(0, dy)

            def go(j=j, dy=dy, qq=qq):
                fcopy(a, qq, (p, q), 0).wait_recv()
                for i, dx in enumerate((1, 3, 2)):
                    fcopy(a, qq, (p, q_at(dx, 0)), 6 + 3 * j + i).start()
            when(needed(a, qq), go)

    def f_wait(a):
        for dx in (1, 3, 2):
            for dy in range(4):
                qq = q_at(dx, dy)
                when(needed(a, qq), lambda qq=qq: fcopy(a, qq, (p, q), 0).wait_recv())

    def f_drain(a):
        def own():
            for i in range(6):
                fcopy(a, q, (p, q), i).wait_send()
        when(needed(a, q), own)
        for j, dy in enumerate((1, 3, 2)):
            qq = q_at(0, dy)

            def go(j=j, qq=qq):
                for i in range(3):
                    fcopy(a, qq, (p, q), 6 + 3 * j + i).wait_send()
            when(needed(a, qq), go)

    def gcopy(s, b, dev):
        return pltpu.make_async_remote_copy(
            src_ref=v.at[s, b], dst_ref=v.at[s, b],
            send_sem=g_send.at[s], recv_sem=g_recv.at[s, b],
            device_id=dev, device_id_type=MESH,
        )

    ydev = (panel_of(1 - yl, z, c), q)
    cdev = (panel_of(yl, z, 1 - c), q)
    ZORDER = (1, 7, 2, 6, 3, 5, 4)

    def g_start(s):
        for d in ZORDER:
            gcopy(s, p, (panel_of(yl, z_at(d), c), q)).start()
        gcopy(s, p, ydev).start()
        gcopy(s, p, cdev).start()

    def g_mid(s):
        for d in ZORDER:
            b = panel_of(yl, z_at(d), c)
            gcopy(s, b, cdev).wait_recv()
            gcopy(s, b, ydev).start()
            gcopy(s, b, cdev).start()

    def g_end(s):
        for d in (0,) + ZORDER:
            b = panel_of(1 - yl, z_at(d), c)
            gcopy(s, b, cdev).wait_recv()
            gcopy(s, b, cdev).start()
        for d in (0,) + ZORDER:
            gcopy(s, panel_of(yl, z_at(d), 1 - c), cdev).wait_recv()
        for d in (0,) + ZORDER:
            gcopy(s, panel_of(1 - yl, z_at(d), 1 - c), cdev).wait_recv()

    def g_drain(s):
        pltpu.make_async_remote_copy(
            src_ref=v.at[s, pl.ds(0, 31)], dst_ref=v.at[s, pl.ds(0, 31)],
            send_sem=g_send.at[s], recv_sem=g_recv.at[s, 0],
            device_id=cdev, device_id_type=MESH,
        ).wait_send()

    lane = lax.broadcasted_iota(jnp.int32, (64, 128), 1)
    low = lane < 64

    def interleave(a0, a1):
        f0, f1 = a0.astype(F32), a1.astype(F32)
        first = jnp.where(low, f0, pltpu.roll(f1, 64, 1)).astype(BF)
        second = jnp.where(low, pltpu.roll(f0, 64, 1), f1).astype(BF)
        return first, second

    def zero_fill(i, _):
        zs = jnp.zeros((2, 64, 128), BF)
        zl = jnp.zeros((2, 128, 128), BF)
        fs[1, pl.ds(2 * i, 2)] = zs
        fs[2, pl.ds(2 * i, 2)] = zs
        fl[0, pl.ds(2 * i, 2)] = zl
        fl[1, pl.ds(2 * i, 2)] = zl
        return 0

    lax.fori_loop(0, NQ, zero_fill, 0)

    for i, ref in ((1, lp_ref), (2, up_ref), (3, uu_ref)):
        first, second = interleave(ref[0], ref[1])
        fs[i, 2 * q] = first
        fs[i, 2 * q + 1] = second
    for i, ref in ((0, pl_ref), (1, pu_ref)):
        fl[i, 2 * q] = ref[:, 0:128]
        fl[i, 2 * q + 1] = ref[:, 128:256]
    v[0, p] = jnp.concatenate([pivot_ref[0], pivot_ref[1]], axis=0).T.astype(BF)

    barrier = pltpu.get_barrier_semaphore()
    for d in range(1, NZ):
        signal((panel_of(yl, z_at(d), c), q), barrier)
    signal(ydev, barrier)
    signal(cdev, barrier)
    for d in range(1, 4):
        signal((p, q_at(0, d)), barrier)
        signal((p, q_at(d, 0)), barrier)
    child = p // 16
    for k in range(2):
        src = 16 * k + t
        pl.when(src != p)(lambda src=src: signal((src, q), barrier))
    self_count = jnp.where(jnp.logical_or(p == 0, p == 31), 1, 0)
    pl.semaphore_wait(barrier, 7 + 2 + 6 + 2 - self_count)

    def mcopies(h):
        dst = 2 * (p - 16 * child) + h
        rows = pl.ds(64 * h, 64)
        a = pltpu.make_async_remote_copy(
            src_ref=lu_ref.at[rows], dst_ref=lu_in.at[child],
            send_sem=m_send.at[0, h], recv_sem=m_recv.at[0, child],
            device_id=(dst, q), device_id_type=MESH,
        )
        b = pltpu.make_async_remote_copy(
            src_ref=update_ref.at[rows], dst_ref=upd_in.at[child],
            send_sem=m_send.at[1, h], recv_sem=m_recv.at[1, child],
            device_id=(dst, q), device_id_type=MESH,
        )
        return dst, a, b

    for h in range(2):
        dst, a, b = mcopies(h)

        @pl.when(dst != p)
        def _():
            a.start()
            b.start()

        @pl.when(dst == p)
        def _():
            lu_in[child] = lu_ref[pl.ds(64 * h, 64), :]
            upd_in[child] = update_ref[pl.ds(64 * h, 64), :]

    g_start(0)

    for k in range(2):
        @pl.when(16 * k + t != p)
        def _():
            for i, ref in ((0, lu_in), (1, upd_in)):
                pltpu.make_async_remote_copy(
                    src_ref=ref.at[k], dst_ref=ref.at[k],
                    send_sem=m_send.at[i, 0], recv_sem=m_recv.at[i, k],
                    device_id=cdev, device_id_type=MESH,
                ).wait_recv()

    first, second = interleave(lu_in[0], lu_in[1])
    fs[0, 2 * q] = first
    fs[0, 2 * q + 1] = second
    y_phase(LU)
    g_mid(0)
    x_phase(LU)
    y_phase(PLO)
    y_phase(LP)
    g_end(0)

    half_mask = (lax.rem(lax.broadcasted_iota(jnp.int32, (64, 512), 1), 128) < 64).astype(F32)
    mask_low = half_mask.astype(BF)
    mask_high = (1.0 - half_mask).astype(BF)

    def wide(ref, lead, i):
        return jnp.concatenate([ref[lead, 4 * i + j] for j in range(4)], axis=1)

    def apply_large(s, a):
        def step(i, acc):
            return acc + dot(wide(v, s, i), wide(fl, a, i), NT)
        return lax.fori_loop(0, NP // 4, step, jnp.zeros((128, 128), F32))

    def apply_small(s, a, init):
        def step(i, acc):
            f = wide(fs, a, i)
            both = jnp.concatenate([f * mask_low, f * mask_high], axis=0)
            return acc + dot(wide(v, s, i), both, NT)
        return lax.fori_loop(0, NP // 4, step, init)

    zero = jnp.zeros((128, 128), F32)

    m0 = maps_ref[pl.ds(t, 1), :]
    m1 = maps_ref[pl.ds(16 + t, 1), :]
    lane1 = lax.broadcasted_iota(jnp.int32, (8, 128), 1)
    m0 = jnp.broadcast_to(m0, (8, 128))
    m1 = jnp.broadcast_to(m1, (8, 128))
    even = c == 0
    lo = jnp.where(even, m0, pltpu.roll(m0, 64, 1))
    hi = jnp.where(even, pltpu.roll(m1, 64, 1), m1)
    m = jnp.where(lane1 < 64, lo, hi)[0:1] - 128 * p
    row = lax.broadcasted_iota(jnp.int32, (128, 128), 0)
    select = jnp.where(row == m, 1.0, 0.0).astype(BF)

    upd_t = jnp.concatenate([upd_in[0], upd_in[1]], axis=0).T
    parent_t = parent_ref[...].T

    f_wait(LU)
    u_t = apply_small(0, 0, upd_t)
    s_t = parent_t + dot(u_t.astype(BF), select, NT)
    v[1, p] = s_t.astype(BF)
    g_start(1)

    x_phase(PLO)
    x_phase(LP)
    y_phase(PUP)
    g_mid(1)
    f_wait(LP)
    v[4, p] = apply_small(0, 1, zero).astype(BF)
    g_end(1)
    f_wait(PLO)
    v[2, p] = apply_large(1, 0).astype(BF)
    g_start(2)
    g_start(4)
    x_phase(PUP)
    y_phase(UP)
    y_phase(UU)
    g_mid(2)
    g_end(2)
    g_mid(4)
    f_wait(PUP)
    sol_t = apply_large(2, 1)
    r_t = dot(sol_t.astype(BF), select, NN)
    v[3, p] = r_t.astype(BF)
    g_start(3)
    sol_ref[...] = sol_t.T
    x_phase(UP)
    x_phase(UU)
    g_end(4)
    f_wait(UP)
    acc = apply_small(4, 2, zero)
    g_mid(3)
    g_end(3)
    f_wait(UU)
    acc = apply_small(3, 3, acc)
    out = acc.T
    child_ref[0] = out[0:64]
    child_ref[1] = out[64:128]

    for s in range(5):
        g_drain(s)
    for a in range(6):
        f_drain(a)
    for h in range(2):
        dst, a, b = mcopies(h)

        @pl.when(dst != p)
        def _():
            a.wait_send()
            b.wait_send()


def shards(pivot_rhs, update_rhs, parent_rhs, lower_pivot, lower_update, parent_lower, parent_upper, upper_pivot, upper_update, maps):
    vm = pl.BlockSpec(memory_space=pltpu.VMEM)
    dma = pltpu.SemaphoreType.DMA
    return pl.pallas_call(
        body,
        out_shape=(
            jax.ShapeDtypeStruct((128, 128), F32),
            jax.ShapeDtypeStruct((2, 64, 128), F32),
        ),
        in_specs=[vm] * 10,
        out_specs=(vm, vm),
        scratch_shapes=[
            pltpu.VMEM((5, NP, 128, 128), BF),
            pltpu.VMEM((4, NP, 64, 128), BF),
            pltpu.VMEM((2, NP, 128, 128), BF),
            pltpu.VMEM((2, 64, 128), BF),
            pltpu.VMEM((2, 64, 128), F32),
            pltpu.VMEM((8, 128), F32),
            dma((5,)),
            dma((5, NP)),
            dma((6, 15)),
            dma((6, NQ)),
            dma((2, 2)),
            dma((2, 2)),
        ],
        compiler_params=pltpu.CompilerParams(collective_id=0, has_side_effects=True, vmem_limit_bytes=32 << 20),
    )(
        pivot_rhs, update_rhs, parent_rhs, lower_pivot, lower_update, parent_lower, parent_upper,
        upper_pivot, upper_update, maps.reshape(32, 128),
    )


def solution(mesh):
    placed = (
        P(None, "panel", "rhs"),
        P("panel", "rhs"),
        P("panel", "rhs"),
        P(None, "panel", "rhs"),
        P("panel", "rhs"),
        P("panel", "rhs"),
        P("panel", "rhs"),
        P(None, "panel", "rhs"),
        P(None, "panel", "rhs"),
        P(),
    )
    return jax.shard_map(
        shards,
        mesh=mesh,
        in_specs=placed,
        out_specs=(P("panel", "rhs"), P(None, "panel", "rhs")),
        check_vma=False,
    )
```

```python
import jax
import jax.numpy as jnp
from jax import lax
from jax.experimental import pallas as pl
from jax.experimental.pallas import tpu as pltpu
from jax.sharding import PartitionSpec as P

MESH = pl.DeviceIdType.MESH
BF = jnp.bfloat16
F32 = jnp.float32
NZ = 8
NT = 16
H = 2
W = 64 // H
CONTRACT_LAST = (((1,), (1,)), ((), ()))
CONTRACT_INNER = (((1,), (0,)), ((), ()))
ZORDER = (1, 7, 2, 6, 3, 5, 4)
TURN = (1, 3, 2)

LU, LP, PLO, PUP, UP, UU = range(6)
X, S, M, R, PM = range(5)


def dot(a, b, dims=CONTRACT_LAST):
    return lax.dot_general(a, b, dims, preferred_element_type=F32)


def body(
    pivot_hbm, update_hbm, parent_hbm, lp_hbm, lu_hbm, pl_hbm, pu_hbm, up_hbm, uu_hbm, maps_hbm,
    sol_ref, child_ref,
    v, f_lu, f_lp, f_pl, f_pu, f_up, f_uu,
    lu_ref, update_ref, pivot_ref, parent_ref, maps_ref,
    upd_in, x_out, x_in, u_out, u_in, par_out, par_in, sol_out, sol_in, ch_out, ch_in, acc_ref,
    g_send, g_recv, y_recv, f_send, f_recv, d_send, d_recv, m_send, m_recv, e_send, e_recv, l_sem,
):
    p = lax.axis_index("panel")
    q = lax.axis_index("rhs")
    c = lax.rem(p, 2)
    t = p // 2
    yl = t // NZ
    z = lax.rem(t, NZ)
    x = q // 4
    yh = lax.rem(q, 4)
    factors = (f_lu, f_lp, f_pl, f_pu, f_up, f_uu)

    def z_at(d):
        return lax.rem(z + d, NZ)

    def q_at(dx, dy):
        return lax.rem(x + dx, 4) * 4 + lax.rem(yh + dy, 4)

    def z_dev(d):
        return ((yl * NZ + z_at(d)) * 2 + c, q)

    y_dev = (((1 - yl) * NZ + z) * 2 + c, q)
    c_dev = (2 * t + 1 - c, q)
    move_src = 16 * c + t
    move_dst = 2 * lax.rem(p, 16) + p // 16
    moves = move_src != p

    pairs = [(lu_hbm, lu_ref), (pivot_hbm, pivot_ref), (update_hbm, update_ref), (parent_hbm, parent_ref), (maps_hbm, maps_ref)]
    pairs += [(h, f.at[q, c]) for h, f in ((lp_hbm, f_lp), (pl_hbm, f_pl), (pu_hbm, f_pu), (up_hbm, f_up), (uu_hbm, f_uu))]
    loads = [pltpu.make_async_copy(a, b, l_sem.at[i]) for i, (a, b) in enumerate(pairs)]
    for load in loads:
        load.start()

    barrier = pltpu.get_barrier_semaphore()

    def signal(dev):
        pl.semaphore_signal(barrier, inc=1, device_id=dev, device_id_type=MESH)

    for d in range(1, NZ):
        signal(z_dev(d))
    signal(y_dev)
    signal(c_dev)
    for d in range(1, 4):
        signal((p, q_at(0, d)))
        signal((p, q_at(d, 0)))
    pl.when(moves)(lambda: signal((move_src, q)))

    def needed(a, qq):
        if a in (LP, PLO):
            return qq <= t
        if a in (PUP, UP):
            return qq >= t
        return None

    def when(cond, fn):
        if cond is None:
            fn()
        else:
            pl.when(cond)(fn)

    def f_copy(a, qq, dev):
        block = factors[a].at[qq, c]
        return pltpu.make_async_remote_copy(
            src_ref=block, dst_ref=block, send_sem=f_send.at[a], recv_sem=f_recv.at[a, qq],
            device_id=dev, device_id_type=MESH,
        )

    def d_copy(a, part):
        block = factors[a].at[part, c]
        return pltpu.make_async_remote_copy(
            src_ref=block, dst_ref=block, send_sem=d_send.at[a], recv_sem=d_recv.at[a],
            device_id=c_dev, device_id_type=MESH,
        )

    def send_x(a, qq):
        for dx in TURN:
            f_copy(a, qq, (p, q_at(dx, 0))).start()

    def f_y(a):
        return [
            lambda dy=dy: when(needed(a, q), f_copy(a, q, (p, q_at(0, dy))).start)
            for dy in TURN
        ]

    def f_x(a):
        def go():
            when(needed(a, q), lambda: send_x(a, q))
            d_copy(a, q).start()
        return [go]

    def f_turn(a):
        def step(qq):
            def go():
                f_copy(a, qq, c_dev).wait_recv()
                send_x(a, qq)
            when(needed(a, qq), go)
            d_copy(a, qq).start()
        return [lambda qq=q_at(0, dy): step(qq) for dy in TURN]

    def f_last(a):
        def step(qq):
            when(needed(a, qq), f_copy(a, qq, c_dev).wait_recv)
            d_copy(a, qq).start()
        return [lambda qq=q_at(dx, dy): step(qq) for dy in (0,) + TURN for dx in TURN]

    def f_ready(a):
        d_copy(a, pl.ds(0, NT)).wait_recv()

    def f_drain(a):
        def sent(n):
            part = factors[a].at[pl.ds(0, 3 * n), 0]
            pltpu.make_async_remote_copy(
                src_ref=part, dst_ref=part, send_sem=f_send.at[a], recv_sem=f_recv.at[a, 0],
                device_id=c_dev, device_id_type=MESH,
            ).wait_send()
        if needed(a, q) is None:
            sent(5)
        else:
            column = t - 4 * x + 1 if a in (LP, PLO) else 4 * x + 4 - t
            count = jnp.clip(column, 0, 4) + jnp.where(needed(a, q), 1, 0)
            for n in range(1, 6):
                pl.when(count == n)(lambda n=n: sent(n))
        d_copy(a, pl.ds(0, NT)).wait_send()

    def run(*steps):
        for group in steps:
            for step in group:
                step()

    def g_copy(s, h, tt, dev, sem):
        block = v.at[s, h, tt]
        return pltpu.make_async_remote_copy(
            src_ref=block, dst_ref=block, send_sem=g_send.at[s, h], recv_sem=sem,
            device_id=dev, device_id_type=MESH,
        )

    def g_start(s, h):
        for d in ZORDER:
            g_copy(s, h, t, z_dev(d), g_recv.at[s, h, z]).start()
        g_copy(s, h, t, y_dev, y_recv.at[s, h]).start()

    def g_turn(s, h, *steps):
        steps = [step for group in steps for step in group]
        for i, d in enumerate(ZORDER):
            tt = yl * NZ + z_at(d)
            g_copy(s, h, tt, y_dev, g_recv.at[s, h, z_at(d)]).wait_recv()
            g_copy(s, h, tt, y_dev, y_recv.at[s, h]).start()
            todo = steps[len(steps) * i // 7 : len(steps) * (i + 1) // 7]
            run(todo)

    def g_last(s, h):
        g_copy(s, h, pl.ds((1 - yl) * NZ, NZ), y_dev, y_recv.at[s, h]).wait_recv()

    def g_drain(s, h):
        g_copy(s, h, pl.ds(0, 15), y_dev, y_recv.at[s, h]).wait_send()

    def e_copy(i, src, dst):
        return pltpu.make_async_remote_copy(
            src_ref=src, dst_ref=dst, send_sem=e_send.at[i], recv_sem=e_recv.at[i],
            device_id=c_dev, device_id_type=MESH,
        )

    mine = pl.ds(pl.multiple_of(64 * c, 64), 64)
    other = pl.ds(pl.multiple_of(64 - 64 * c, 64), 64)
    x_ex = e_copy(0, x_out.at[other], x_in)
    u_ex = e_copy(1, u_out.at[other], u_in)
    par_ex = e_copy(2, par_out.at[other], par_in)
    sol_ex = e_copy(3, sol_out, sol_in)
    ch_ex = e_copy(4, ch_out, ch_in)

    first_core = c == 0

    def ordered(own, got):
        return jnp.where(first_core, own, got), jnp.where(first_core, got, own)

    low = lax.broadcasted_iota(jnp.int32, (64, 128), 1) < 64

    def swap_halves(a, b):
        return jnp.where(low, a, pltpu.roll(b, 64, 1)), jnp.where(low, pltpu.roll(a, 64, 1), b)

    with jax.named_scope("prep"):
        loads[1].wait()
        x_out[...] = jnp.concatenate([pivot_ref[0], pivot_ref[1]], axis=0).T.astype(BF).astype(F32)

        def clear(f, i):
            @pl.when(i != q)
            def _():
                f[i, c] = jnp.zeros(f.shape[2:], BF)

        def zero_fill(i, _):
            @pl.when(i > t)
            def _():
                clear(f_lp, i)
                clear(f_pl, i)

            @pl.when(i < t)
            def _():
                clear(f_up, i)
                clear(f_pu, i)

            return 0

        lax.fori_loop(0, NT, zero_fill, 0)
        loads[0].wait()
    with jax.named_scope("barrier"):
        pl.semaphore_wait(barrier, 7 + 2 + 6 + jnp.where(moves, 1, 0))

    own_lu = f_lu.at[q, c]
    lu_move = pltpu.make_async_remote_copy(
        src_ref=lu_ref, dst_ref=f_lu.at[q, p // 16], send_sem=m_send.at[0], recv_sem=m_recv.at[0],
        device_id=(move_dst, q), device_id_type=MESH,
    )
    upd_move = pltpu.make_async_remote_copy(
        src_ref=update_ref, dst_ref=upd_in, send_sem=m_send.at[1], recv_sem=m_recv.at[1],
        device_id=(move_dst, q), device_id_type=MESH,
    )
    lu_arrival = pltpu.make_async_remote_copy(
        src_ref=own_lu, dst_ref=own_lu, send_sem=m_send.at[0], recv_sem=m_recv.at[0],
        device_id=c_dev, device_id_type=MESH,
    )
    x_ex.start()
    pl.when(moves)(lu_move.start)

    @pl.when(jnp.logical_not(moves))
    def _():
        f_lu[q, c] = lu_ref[...]

    with jax.named_scope("x_ex"):
        x_ex.wait_recv()
    x0, x1 = swap_halves(*ordered(x_out[mine, :], x_in[...]))
    xt = jnp.concatenate([x0, x1], axis=1).astype(BF)
    for h in range(H):
        v[X, h, t] = xt[W * h : W * (h + 1)]
        g_start(X, h)

    for load in loads[2:]:
        load.wait()
    run(f_x(PLO), f_x(LP), f_x(PUP))
    pl.when(moves)(upd_move.start)

    @pl.when(jnp.logical_not(moves))
    def _():
        upd_in[...] = update_ref[...]

    par_out[...] = parent_ref[...].T
    par_ex.start()
    with jax.named_scope("w_lu_move"):
        pl.when(moves)(lu_arrival.wait_recv)
    run(f_y(LU), f_x(LU))
    with jax.named_scope("x_turn0"):
        g_turn(X, 0, f_y(PLO), f_turn(LU))
    with jax.named_scope("x_turn1"):
        for h in range(1, H):
            g_turn(X, h)
    with jax.named_scope("w_upd"):
        pl.when(moves)(upd_move.wait_recv)
        u_out[...] = upd_in[...].T
    u_ex.start()

    row = lax.broadcasted_iota(jnp.int32, (256, 128), 0)

    def selection(k):
        return jnp.where(row == maps_ref[pl.ds(16 * k + t, 1), :] - 256 * t, 1.0, 0.0).astype(BF)

    select = (selection(0), selection(1))

    def line(s, h, side):
        first = side * NZ
        return [v[s, h, first + j] for j in range(NZ)], [first + j for j in range(NZ)]

    def apply_parent(s, h, f, side):
        blocks, at = line(s, h, side)
        left = jnp.concatenate(blocks, axis=1)
        right = jnp.concatenate([f[i].reshape(256, 256) for i in at], axis=1)
        return dot(left, right)

    def apply_child(s, h, f, side):
        blocks, at = line(s, h, side)
        out = []
        for k in range(2):
            left = jnp.concatenate([b[:, 128 * k : 128 * (k + 1)] for b in blocks], axis=1)
            if f is f_lu:
                right = jnp.concatenate([f[i, k] for i in at], axis=1)
            else:
                right = jnp.concatenate(
                    [jnp.concatenate([f[i, 0, k], f[i, 1, k]], axis=0) for i in at], axis=1
                )
            out.append(dot(left, right))
        return jnp.concatenate(out, axis=1)

    def both(fn, s, h, f):
        return fn(s, h, f, yl) + fn(s, h, f, 1 - yl)

    run(f_y(LP))
    with jax.named_scope("lu_last"):
        run(f_last(LU)[:6], f_y(PUP), f_last(LU)[6:])
    with jax.named_scope("pl_turn"):
        run(f_turn(PLO))
    with jax.named_scope("x_last"):
        g_last(X, 0)
    with jax.named_scope("lu_ready"):
        f_ready(LU)
    with jax.named_scope("ex_upd_par"):
        par_ex.wait_recv()
        u_ex.wait_recv()
    upd = ordered(u_out[mine, :], u_in[...])
    par = jnp.concatenate(ordered(par_out[mine, :], par_in[...]), axis=1)
    for h in range(H):
        rows = slice(W * h, W * (h + 1))
        if h:
            with jax.named_scope("x_last1"):
                g_last(X, h)
        with jax.named_scope("mm_s"):
            u = both(apply_child, X, h, f_lu)
            u0 = (upd[0][rows] + u[:, :128]).astype(BF)
            u1 = (upd[1][rows] + u[:, 128:]).astype(BF)
            st = par[rows] + (dot(u0, select[0]) + dot(u1, select[1]))
            v[S, h, t] = st.astype(BF)
        g_start(S, h)

    def stage(src, f, a, steps, finish):
        steps = steps if H == 2 else [steps[0] + steps[1]]
        for h in range(H):
            with jax.named_scope("turn%d_%d" % (h, src)):
                g_turn(src, h, steps[h])
        with jax.named_scope("f_last_%d" % src):
            run(f_last(a))
        with jax.named_scope("f_ready_%d" % src):
            f_ready(a)
        for h in range(H):
            with jax.named_scope("mm0_%d" % src):
                acc_ref[...] = apply_parent(src, h, f, yl)
            with jax.named_scope("last%d_%d" % (h, src)):
                g_last(src, h)
            with jax.named_scope("mm1_%d" % src):
                finish(h, acc_ref[...] + apply_parent(src, h, f, 1 - yl))

    def finish_m(h, acc):
        v[M, h, t] = acc.astype(BF)
        g_start(M, h)

    stage(S, f_pl, PLO, [f_turn(LP) + f_x(UP) + f_x(UU), f_y(UP) + f_turn(PUP)], finish_m)

    with jax.named_scope("lp_last"):
        run(f_last(LP))
        f_ready(LP)
    for h in range(H):
        with jax.named_scope("mm_p"):
            v[PM, h, t] = both(apply_child, X, h, f_lp).astype(BF)
        g_start(PM, h)
    sols = []

    def finish_r(h, acc):
        half = acc.astype(BF)
        r = [dot(half, select[k], CONTRACT_INNER) for k in range(2)]
        v[R, h, t] = jnp.concatenate(r, axis=1).astype(BF)
        g_start(R, h)
        sols.append(acc)

    stage(M, f_pu, PUP, [f_y(UU), f_turn(UP)], finish_r)

    sol = jnp.concatenate(sols, axis=0)
    own_sol, their_sol = ordered(sol[:, :128], sol[:, 128:])
    sol_out[...] = their_sol
    sol_ex.start()
    with jax.named_scope("u_turn"):
        run(f_turn(UU))
    with jax.named_scope("p_turn"):
        for h in range(H):
            g_turn(PM, h)
    for h in range(H):
        with jax.named_scope("turn%d_R" % h):
            g_turn(R, h, f_last(UP)[12 // H * h : 12 // H * (h + 1)])
    with jax.named_scope("uu_last"):
        run(f_last(UU))
    with jax.named_scope("p_last"):
        for h in range(H):
            g_last(PM, h)
    with jax.named_scope("up_ready"):
        f_ready(UP)
        f_ready(UU)
    outs = []
    for h in range(H):
        with jax.named_scope("mm_c0"):
            acc_ref[...] = both(apply_child, PM, h, f_up) + apply_child(R, h, f_uu, yl)
        with jax.named_scope("r_last%d" % h):
            g_last(R, h)
        with jax.named_scope("mm_c1"):
            outs.append(acc_ref[...] + apply_child(R, h, f_uu, 1 - yl))
    ch = jnp.concatenate(outs, axis=0)
    own_ch, their_ch = ordered(*swap_halves(ch[:, :128], ch[:, 128:]))
    ch_out[...] = their_ch
    ch_ex.start()
    with jax.named_scope("fin_sol"):
        sol_ex.wait_recv()
        sol_ref[...] = jnp.concatenate(ordered(own_sol, sol_in[...]), axis=0).T
    with jax.named_scope("drain"):
        for s in range(5):
            for h in range(H):
                g_drain(s, h)
        for a in range(6):
            f_drain(a)
        pl.when(moves)(lu_move.wait_send)
        pl.when(moves)(upd_move.wait_send)
        for e in (x_ex, u_ex, par_ex, sol_ex, ch_ex):
            e.wait_send()
    with jax.named_scope("fin_ch"):
        ch_ex.wait_recv()
        out = jnp.concatenate(ordered(own_ch, ch_in[...]), axis=0).T
        child_ref[0] = out[0:64]
        child_ref[1] = out[64:128]


def shards(pivot_rhs, update_rhs, parent_rhs, lower_pivot, lower_update, parent_lower, parent_upper, upper_pivot, upper_update, maps):
    vm = pl.BlockSpec(memory_space=pltpu.VMEM)
    dma = pltpu.SemaphoreType.DMA
    square = pltpu.VMEM((128, 128), F32)
    half = pltpu.VMEM((64, 128), F32)
    child_factor = pltpu.VMEM((NT, 2, 2, 64, 128), BF)
    parent_factor = pltpu.VMEM((NT, 2, 128, 256), BF)
    return pl.pallas_call(
        body,
        out_shape=(
            jax.ShapeDtypeStruct((128, 128), F32),
            jax.ShapeDtypeStruct((2, 64, 128), F32),
        ),
        in_specs=[pl.BlockSpec(memory_space=pltpu.HBM)] * 10,
        out_specs=(vm, vm),
        scratch_shapes=[
            pltpu.VMEM((5, H, NT, W, 256), BF),
            pltpu.VMEM((NT, 2, 128, 128), BF),
            child_factor,
            parent_factor,
            parent_factor,
            child_factor,
            child_factor,
            pltpu.VMEM((128, 128), BF),
            square,
            pltpu.VMEM((2, 64, 128), F32),
            square,
            pltpu.VMEM((32, 128), jnp.int32),
            square, square, half, square, half, square, half, half, half, half, half,
            pltpu.VMEM((W, 256), F32),
            dma((5, H)),
            dma((5, H, NZ)),
            dma((5, H)),
            dma((6,)),
            dma((6, NT)),
            dma((6,)),
            dma((6,)),
            dma((2,)),
            dma((2,)),
            dma((5,)),
            dma((5,)),
            dma((10,)),
        ],
        compiler_params=pltpu.CompilerParams(collective_id=0, has_side_effects=True, vmem_limit_bytes=60 << 20),
    )(
        pivot_rhs, update_rhs, parent_rhs, lower_pivot, lower_update, parent_lower, parent_upper,
        upper_pivot, upper_update, maps.reshape(32, 128),
    )


def solution(mesh):
    placed = (
        P(None, "panel", "rhs"),
        P("panel", "rhs"),
        P("panel", "rhs"),
        P(None, "panel", "rhs"),
        P("panel", "rhs"),
        P("panel", "rhs"),
        P("panel", "rhs"),
        P(None, "panel", "rhs"),
        P(None, "panel", "rhs"),
        P(),
    )
    return jax.shard_map(
        shards,
        mesh=mesh,
        in_specs=placed,
        out_specs=(P("panel", "rhs"), P(None, "panel", "rhs")),
        check_vma=False,
    )
```

```python
import jax
import jax.numpy as jnp
from jax import lax
from jax.experimental import pallas as pl
from jax.experimental.pallas import tpu as pltpu
from jax.sharding import PartitionSpec as P

MESH = pl.DeviceIdType.MESH
BF = jnp.bfloat16
F32 = jnp.float32
NZ = 8
NT = 16
H = 2
W = 64 // H
CONTRACT_LAST = (((1,), (1,)), ((), ()))
CONTRACT_INNER = (((1,), (0,)), ((), ()))
NEAR = (2, 6, 1, 7)
TURN = (1, 3, 2)

LU, LP, PLO, PUP, UP, UU = range(6)
X, S, M, R, PM = range(5)
SLOT = (0, 1, 0, 1, 2)


def dot(a, b, dims=CONTRACT_LAST):
    return lax.dot_general(a, b, dims, preferred_element_type=F32)


def body(
    pivot_hbm, update_hbm, parent_hbm, lp_hbm, lu_hbm, pl_hbm, pu_hbm, up_hbm, uu_hbm, maps_hbm,
    sol_ref, child_ref,
    v, f_lu, f_lp, f_pl, f_pu, f_up, f_uu,
    lu_ref, update_ref, pivot_ref, parent_ref, maps_ref,
    upd_in, x_out, x_in, u_out, u_in, par_out, par_in, sol_out, sol_in, ch_out, ch_in, acc_ref,
    g_send, g_recv, y_recv, f_send, f_recv, d_send, d_recv, m_send, m_recv, e_send, e_recv, l_sem,
):
    p = lax.axis_index("panel")
    q = lax.axis_index("rhs")
    c = lax.rem(p, 2)
    first_core = c == 0
    t = p // 2
    yl = t // NZ
    z = lax.rem(t, NZ)
    x = q // 4
    yh = lax.rem(q, 4)
    factors = (f_lu, f_lp, f_pl, f_pu, f_up, f_uu)

    def z_at(d):
        return lax.rem(z + d, NZ)

    def q_at(dx, dy):
        return lax.rem(x + dx, 4) * 4 + lax.rem(yh + dy, 4)

    def z_dev(d):
        return ((yl * NZ + z_at(d)) * 2 + c, q)

    def diagonal(d):
        return (((1 - yl) * NZ + z_at(d)) * 2 + c, q)

    y_dev = (((1 - yl) * NZ + z) * 2 + c, q)
    c_dev = (2 * t + 1 - c, q)
    move_src = 16 * c + t
    move_dst = 2 * lax.rem(p, 16) + p // 16
    moves = move_src != p

    pairs = [(lu_hbm, lu_ref), (pivot_hbm, pivot_ref), (update_hbm, update_ref), (parent_hbm, parent_ref), (maps_hbm, maps_ref)]
    pairs += [(h, f.at[q, c]) for h, f in ((lp_hbm, f_lp), (pl_hbm, f_pl), (pu_hbm, f_pu), (up_hbm, f_up), (uu_hbm, f_uu))]
    loads = [pltpu.make_async_copy(a, b, l_sem.at[i]) for i, (a, b) in enumerate(pairs)]
    for load in loads:
        load.start()

    barrier = pltpu.get_barrier_semaphore()

    def signal(dev):
        pl.semaphore_signal(barrier, inc=1, device_id=dev, device_id_type=MESH)

    for d in NEAR:
        signal(z_dev(d))
        signal(diagonal(d))
    signal(y_dev)
    signal(c_dev)
    for d in range(1, 4):
        signal((p, q_at(0, d)))
        signal((p, q_at(d, 0)))
    pl.when(moves)(lambda: signal((move_src, q)))

    def needed(a, qq):
        if a in (LP, PLO):
            return qq <= t
        if a in (PUP, UP):
            return qq >= t
        return None

    def when(cond, fn):
        if cond is None:
            fn()
        else:
            pl.when(cond)(fn)

    def f_copy(a, qq, dev):
        block = factors[a].at[qq, c]
        return pltpu.make_async_remote_copy(
            src_ref=block, dst_ref=block, send_sem=f_send.at[a], recv_sem=f_recv.at[a, qq],
            device_id=dev, device_id_type=MESH,
        )

    def d_copy(a, part):
        block = factors[a].at[part, c]
        return pltpu.make_async_remote_copy(
            src_ref=block, dst_ref=block, send_sem=d_send.at[a], recv_sem=d_recv.at[a],
            device_id=c_dev, device_id_type=MESH,
        )

    def send_x(a, qq):
        for dx in TURN:
            f_copy(a, qq, (p, q_at(dx, 0))).start()

    def f_y(a):
        return [
            lambda dy=dy: when(needed(a, q), f_copy(a, q, (p, q_at(0, dy))).start)
            for dy in TURN
        ]

    def f_x(a):
        def go():
            when(needed(a, q), lambda: send_x(a, q))
            d_copy(a, q).start()
        return [go]

    def f_turn(a):
        def step(qq):
            def go():
                f_copy(a, qq, c_dev).wait_recv()
                send_x(a, qq)
            when(needed(a, qq), go)
            d_copy(a, qq).start()
        return [lambda qq=q_at(0, dy): step(qq) for dy in TURN]

    def f_last(a):
        def step(qq):
            when(needed(a, qq), f_copy(a, qq, c_dev).wait_recv)
            d_copy(a, qq).start()
        return [lambda qq=q_at(dx, dy): step(qq) for dy in (0,) + TURN for dx in TURN]

    def f_ready(a):
        d_copy(a, pl.ds(0, NT)).wait_recv()

    def f_drain(a):
        def sent(n):
            part = factors[a].at[pl.ds(0, 3 * n), 0]
            pltpu.make_async_remote_copy(
                src_ref=part, dst_ref=part, send_sem=f_send.at[a], recv_sem=f_recv.at[a, 0],
                device_id=c_dev, device_id_type=MESH,
            ).wait_send()
        if needed(a, q) is None:
            sent(5)
        else:
            column = t - 4 * x + 1 if a in (LP, PLO) else 4 * x + 4 - t
            count = jnp.clip(column, 0, 4) + jnp.where(needed(a, q), 1, 0)
            for n in range(1, 6):
                pl.when(count == n)(lambda n=n: sent(n))
        d_copy(a, pl.ds(0, NT)).wait_send()

    def run(*steps):
        for group in steps:
            for step in group:
                step()

    def g_copy(s, h, tt, dev, sem):
        block = v.at[s, h, tt]
        return pltpu.make_async_remote_copy(
            src_ref=block, dst_ref=block, send_sem=g_send.at[0], recv_sem=sem,
            device_id=dev, device_id_type=MESH,
        )

    def g_start(s, h):
        for d in NEAR:
            g_copy(s, h, t, z_dev(d), g_recv.at[SLOT[s], h, NEAR.index(NZ - d)]).start()
        g_copy(s, h, t, y_dev, y_recv.at[s, h]).start()

    def g_turn(s, h, steps=()):
        far = g_recv.at[SLOT[s], h, 4]
        for i, d in enumerate(NEAR):
            tt = yl * NZ + z_at(d)
            g_copy(s, h, tt, y_dev, g_recv.at[SLOT[s], h, i]).wait_recv()

            def relay(e):
                g_copy(s, h, tt, z_dev(e), far).start()
                g_copy(s, h, tt, diagonal(e), y_recv.at[s, h]).start()

            if d == 2:
                relay(7)
                pl.when(first_core)(lambda: relay(6))
            if d == 6:
                relay(1)
                pl.when(jnp.logical_not(first_core))(lambda: relay(2))
            g_copy(s, h, tt, y_dev, y_recv.at[s, h]).start()
            run(steps[len(steps) * i // 4 : len(steps) * (i + 1) // 4])

    def g_far(s, h):
        g_copy(s, h, pl.ds(0, 3), y_dev, g_recv.at[SLOT[s], h, 4]).wait_recv()

    def turns(s, *steps):
        for h in range(H):
            with jax.named_scope("near%d_%d" % (h, s)):
                g_turn(s, h, steps[h] if h < len(steps) else ())

    def fars(s):
        for h in range(H):
            with jax.named_scope("far%d_%d" % (h, s)):
                g_far(s, h)

    def g_last(s, h):
        g_copy(s, h, pl.ds((1 - yl) * NZ, NZ), y_dev, y_recv.at[s, h]).wait_recv()

    def g_drain():
        part = v.at[:, :, pl.ds(0, 15)]
        pltpu.make_async_remote_copy(
            src_ref=part, dst_ref=part, send_sem=g_send.at[0], recv_sem=y_recv.at[0, 0],
            device_id=y_dev, device_id_type=MESH,
        ).wait_send()

    def e_copy(i, src, dst):
        return pltpu.make_async_remote_copy(
            src_ref=src, dst_ref=dst, send_sem=e_send.at[i], recv_sem=e_recv.at[i],
            device_id=c_dev, device_id_type=MESH,
        )

    mine = pl.ds(pl.multiple_of(64 * c, 64), 64)
    other = pl.ds(pl.multiple_of(64 - 64 * c, 64), 64)
    x_ex = e_copy(0, x_out.at[other], x_in)
    u_ex = e_copy(1, u_out.at[other], u_in)
    par_ex = e_copy(2, par_out.at[other], par_in)
    sol_ex = e_copy(3, sol_out, sol_in)
    ch_ex = e_copy(4, ch_out, ch_in)


    def ordered(own, got):
        return jnp.where(first_core, own, got), jnp.where(first_core, got, own)

    low = lax.broadcasted_iota(jnp.int32, (64, 128), 1) < 64

    def swap_halves(a, b):
        return jnp.where(low, a, pltpu.roll(b, 64, 1)), jnp.where(low, pltpu.roll(a, 64, 1), b)

    with jax.named_scope("prep"):
        loads[1].wait()
        x_out[...] = jnp.concatenate([pivot_ref[0], pivot_ref[1]], axis=0).T.astype(BF).astype(F32)

        loads[0].wait()
    with jax.named_scope("barrier"):
        pl.semaphore_wait(barrier, 8 + 2 + 6 + jnp.where(moves, 1, 0))

    own_lu = f_lu.at[q, c]
    lu_move = pltpu.make_async_remote_copy(
        src_ref=lu_ref, dst_ref=f_lu.at[q, p // 16], send_sem=m_send.at[0], recv_sem=m_recv.at[0],
        device_id=(move_dst, q), device_id_type=MESH,
    )
    upd_move = pltpu.make_async_remote_copy(
        src_ref=update_ref, dst_ref=upd_in, send_sem=m_send.at[1], recv_sem=m_recv.at[1],
        device_id=(move_dst, q), device_id_type=MESH,
    )
    lu_arrival = pltpu.make_async_remote_copy(
        src_ref=own_lu, dst_ref=own_lu, send_sem=m_send.at[0], recv_sem=m_recv.at[0],
        device_id=c_dev, device_id_type=MESH,
    )
    x_ex.start()
    pl.when(moves)(lu_move.start)

    @pl.when(jnp.logical_not(moves))
    def _():
        f_lu[q, c] = lu_ref[...]

    with jax.named_scope("x_ex"):
        x_ex.wait_recv()
    x0, x1 = swap_halves(*ordered(x_out[mine, :], x_in[...]))
    xt = jnp.concatenate([x0, x1], axis=1).astype(BF)
    for h in range(H):
        v[X, h, t] = xt[W * h : W * (h + 1)]
        g_start(X, h)

    for load in loads[2:]:
        load.wait()
    run(f_x(PLO), f_x(LP), f_x(PUP))
    def clear(f, i):
        @pl.when(i != q)
        def _():
            f[i, c] = jnp.zeros(f.shape[2:], BF)

    def zero_fill(i, _):
        @pl.when(i > t)
        def _():
            clear(f_lp, i)
            clear(f_pl, i)

        @pl.when(i < t)
        def _():
            clear(f_up, i)
            clear(f_pu, i)

        return 0

    lax.fori_loop(0, NT, zero_fill, 0)
    pl.when(moves)(upd_move.start)

    @pl.when(jnp.logical_not(moves))
    def _():
        upd_in[...] = update_ref[...]

    par_out[...] = parent_ref[...].T
    par_ex.start()
    with jax.named_scope("w_lu_move"):
        pl.when(moves)(lu_arrival.wait_recv)
    run(f_y(LU), f_x(LU))
    turns(X, f_y(PLO), f_turn(LU))
    fars(X)
    with jax.named_scope("w_upd"):
        pl.when(moves)(upd_move.wait_recv)
        u_out[...] = upd_in[...].T
    u_ex.start()

    row = lax.broadcasted_iota(jnp.int32, (256, 128), 0)

    def selection(k):
        return jnp.where(row == maps_ref[pl.ds(16 * k + t, 1), :] - 256 * t, 1.0, 0.0).astype(BF)

    select = (selection(0), selection(1))

    def line(s, h, side):
        first = side * NZ
        return [v[s, h, first + j] for j in range(NZ)], [first + j for j in range(NZ)]

    def apply_parent(s, h, f, side):
        blocks, at = line(s, h, side)
        left = jnp.concatenate(blocks, axis=1)
        right = jnp.concatenate([f[i].reshape(256, 256) for i in at], axis=1)
        return dot(left, right)

    def apply_child(s, h, f, side):
        blocks, at = line(s, h, side)
        out = []
        for k in range(2):
            left = jnp.concatenate([b[:, 128 * k : 128 * (k + 1)] for b in blocks], axis=1)
            if f is f_lu:
                right = jnp.concatenate([f[i, k] for i in at], axis=1)
            else:
                right = jnp.concatenate(
                    [jnp.concatenate([f[i, 0, k], f[i, 1, k]], axis=0) for i in at], axis=1
                )
            out.append(dot(left, right))
        return jnp.concatenate(out, axis=1)

    def both(fn, s, h, f):
        return fn(s, h, f, yl) + fn(s, h, f, 1 - yl)

    run(f_y(LP))
    with jax.named_scope("lu_last"):
        run(f_last(LU)[:6], f_y(PUP), f_last(LU)[6:])
    with jax.named_scope("pl_turn"):
        run(f_turn(PLO))
    with jax.named_scope("x_last"):
        g_last(X, 0)
    with jax.named_scope("lu_ready"):
        f_ready(LU)
    with jax.named_scope("ex_upd_par"):
        par_ex.wait_recv()
        u_ex.wait_recv()
    upd = ordered(u_out[mine, :], u_in[...])
    par = jnp.concatenate(ordered(par_out[mine, :], par_in[...]), axis=1)
    for h in range(H):
        rows = slice(W * h, W * (h + 1))
        if h:
            with jax.named_scope("x_last1"):
                g_last(X, h)
        with jax.named_scope("mm_s"):
            u = both(apply_child, X, h, f_lu)
            u0 = (upd[0][rows] + u[:, :128]).astype(BF)
            u1 = (upd[1][rows] + u[:, 128:]).astype(BF)
            st = par[rows] + (dot(u0, select[0]) + dot(u1, select[1]))
            v[S, h, t] = st.astype(BF)
        g_start(S, h)

    def stage(src, f, a, steps, finish):
        turns(src, *steps[:2])
        with jax.named_scope("f_last_%d" % src):
            run(f_last(a))
        run(*steps[2:])
        fars(src)
        with jax.named_scope("f_ready_%d" % src):
            f_ready(a)
        with jax.named_scope("mm0_%d" % src):
            for h in range(H):
                acc_ref[h] = apply_parent(src, h, f, yl)
        for h in range(H):
            if h == 0 and src == M:
                with jax.named_scope("uu_turn"):
                    run(f_turn(UU))
            with jax.named_scope("last%d_%d" % (h, src)):
                g_last(src, h)
            with jax.named_scope("mm1_%d" % src):
                finish(h, acc_ref[h] + apply_parent(src, h, f, 1 - yl))

    def finish_m(h, acc):
        v[M, h, t] = acc.astype(BF)
        g_start(M, h)

    stage(S, f_pl, PLO, [f_turn(LP) + f_x(UP) + f_x(UU), f_turn(PUP), f_y(UP)], finish_m)

    sols = []

    def finish_r(h, acc):
        half = acc.astype(BF)
        r = [dot(half, select[k], CONTRACT_INNER) for k in range(2)]
        v[R, h, t] = jnp.concatenate(r, axis=1).astype(BF)
        g_start(R, h)
        sols.append(acc)

    def pm_start():
        with jax.named_scope("lp_last"):
            run(f_last(LP))
            f_ready(LP)
        for h in range(H):
            with jax.named_scope("mm_p"):
                v[PM, h, t] = both(apply_child, X, h, f_lp).astype(BF)
            g_start(PM, h)

    def pm_near():
        with jax.named_scope("pm_near"):
            for h in range(H):
                g_turn(PM, h)

    run(f_y(UU))
    stage(M, f_pu, PUP, [[], f_turn(UP), [pm_start]], finish_r)
    pm_near()

    sol = jnp.concatenate(sols, axis=0)
    own_sol, their_sol = ordered(sol[:, :128], sol[:, 128:])
    sol_out[...] = their_sol
    sol_ex.start()
    turns(R, f_last(UP), f_last(UU))
    fars(R)
    with jax.named_scope("pm_far"):
        for h in range(H):
            g_far(PM, h)
    with jax.named_scope("p_last"):
        for h in range(H):
            g_last(PM, h)
    with jax.named_scope("up_ready"):
        f_ready(UP)
        f_ready(UU)
    outs = []
    with jax.named_scope("mm_c0"):
        for h in range(H):
            acc_ref[h] = both(apply_child, PM, h, f_up) + apply_child(R, h, f_uu, yl)
    for h in range(H):
        with jax.named_scope("r_last%d" % h):
            g_last(R, h)
        with jax.named_scope("mm_c1"):
            outs.append(acc_ref[h] + apply_child(R, h, f_uu, 1 - yl))
    ch = jnp.concatenate(outs, axis=0)
    own_ch, their_ch = ordered(*swap_halves(ch[:, :128], ch[:, 128:]))
    ch_out[...] = their_ch
    ch_ex.start()
    with jax.named_scope("fin_sol"):
        sol_ex.wait_recv()
        sol_ref[...] = jnp.concatenate(ordered(own_sol, sol_in[...]), axis=0).T
    with jax.named_scope("drain"):
        g_drain()
        for a in range(6):
            f_drain(a)
        pl.when(moves)(lu_move.wait_send)
        pl.when(moves)(upd_move.wait_send)
        for e in (x_ex, u_ex, par_ex, sol_ex, ch_ex):
            e.wait_send()
    with jax.named_scope("fin_ch"):
        ch_ex.wait_recv()
        out = jnp.concatenate(ordered(own_ch, ch_in[...]), axis=0).T
        child_ref[0] = out[0:64]
        child_ref[1] = out[64:128]


def shards(pivot_rhs, update_rhs, parent_rhs, lower_pivot, lower_update, parent_lower, parent_upper, upper_pivot, upper_update, maps):
    vm = pl.BlockSpec(memory_space=pltpu.VMEM)
    dma = pltpu.SemaphoreType.DMA
    square = pltpu.VMEM((128, 128), F32)
    half = pltpu.VMEM((64, 128), F32)
    child_factor = pltpu.VMEM((NT, 2, 2, 64, 128), BF)
    parent_factor = pltpu.VMEM((NT, 2, 128, 256), BF)
    return pl.pallas_call(
        body,
        out_shape=(
            jax.ShapeDtypeStruct((128, 128), F32),
            jax.ShapeDtypeStruct((2, 64, 128), F32),
        ),
        in_specs=[pl.BlockSpec(memory_space=pltpu.HBM)] * 10,
        out_specs=(vm, vm),
        scratch_shapes=[
            pltpu.VMEM((5, H, NT, W, 256), BF),
            pltpu.VMEM((NT, 2, 128, 128), BF),
            child_factor,
            parent_factor,
            parent_factor,
            child_factor,
            child_factor,
            pltpu.VMEM((128, 128), BF),
            square,
            pltpu.VMEM((2, 64, 128), F32),
            square,
            pltpu.VMEM((32, 128), jnp.int32),
            square, square, half, square, half, square, half, half, half, half, half,
            pltpu.VMEM((H, W, 256), F32),
            dma((1,)),
            dma((3, H, 5)),
            dma((5, H)),
            dma((6,)),
            dma((6, NT)),
            dma((6,)),
            dma((6,)),
            dma((2,)),
            dma((2,)),
            dma((5,)),
            dma((5,)),
            dma((10,)),
        ],
        compiler_params=pltpu.CompilerParams(collective_id=0, has_side_effects=True, vmem_limit_bytes=60 << 20),
    )(
        pivot_rhs, update_rhs, parent_rhs, lower_pivot, lower_update, parent_lower, parent_upper,
        upper_pivot, upper_update, maps.reshape(32, 128),
    )


def solution(mesh):
    placed = (
        P(None, "panel", "rhs"),
        P("panel", "rhs"),
        P("panel", "rhs"),
        P(None, "panel", "rhs"),
        P("panel", "rhs"),
        P("panel", "rhs"),
        P("panel", "rhs"),
        P(None, "panel", "rhs"),
        P(None, "panel", "rhs"),
        P(),
    )
    return jax.shard_map(
        shards,
        mesh=mesh,
        in_specs=placed,
        out_specs=(P("panel", "rhs"), P(None, "panel", "rhs")),
        check_vma=False,
    )
```

```python
import jax
import jax.numpy as jnp
from jax import lax
from jax.experimental import pallas as pl
from jax.experimental.pallas import tpu as pltpu
from jax.sharding import PartitionSpec as P

MESH = pl.DeviceIdType.MESH
BF = jnp.bfloat16
F32 = jnp.float32
NZ = 8
NT = 16
H = 2
W = 64 // H
CONTRACT_LAST = (((1,), (1,)), ((), ()))
CONTRACT_INNER = (((1,), (0,)), ((), ()))
NEAR = (2, 6, 1, 7)
TURN = (1, 3, 2)

LU, LP, PLO, PUP, UP, UU = range(6)
X, S, M, R, PM = range(5)
SLOT = (0, 1, 0, 1, 2)


def dot(a, b, dims=CONTRACT_LAST):
    return lax.dot_general(a, b, dims, preferred_element_type=F32)


def body(
    pivot_hbm, update_hbm, parent_hbm, lp_hbm, lu_hbm, pl_hbm, pu_hbm, up_hbm, uu_hbm, maps_hbm,
    sol_ref, child_ref,
    v, f_lu, f_lp, f_pl, f_pu, f_up, f_uu,
    lu_ref, update_ref, pivot_ref, parent_ref, maps_ref,
    upd_in, x_out, x_in, u_out, u_in, par_out, par_in, sol_out, sol_in, ch_out, ch_in, acc_ref,
    g_send, g_recv, y_recv, f_send, f_recv, d_send, d_recv, m_send, m_recv, e_send, e_recv, l_sem,
):
    p = lax.axis_index("panel")
    q = lax.axis_index("rhs")
    c = lax.rem(p, 2)
    first_core = c == 0
    t = p // 2
    yl = t // NZ
    z = lax.rem(t, NZ)
    x = q // 4
    yh = lax.rem(q, 4)
    factors = (f_lu, f_lp, f_pl, f_pu, f_up, f_uu)

    def z_at(d):
        return lax.rem(z + d, NZ)

    def q_at(dx, dy):
        return lax.rem(x + dx, 4) * 4 + lax.rem(yh + dy, 4)

    def z_dev(d):
        return ((yl * NZ + z_at(d)) * 2 + c, q)

    def diagonal(d):
        return (((1 - yl) * NZ + z_at(d)) * 2 + c, q)

    y_dev = (((1 - yl) * NZ + z) * 2 + c, q)
    c_dev = (2 * t + 1 - c, q)
    move_src = 16 * c + t
    move_dst = 2 * lax.rem(p, 16) + p // 16
    moves = move_src != p

    pairs = [(lu_hbm, lu_ref), (pivot_hbm, pivot_ref), (update_hbm, update_ref), (parent_hbm, parent_ref), (maps_hbm, maps_ref)]
    pairs += [(h, f.at[q, c]) for h, f in ((lp_hbm, f_lp), (pl_hbm, f_pl), (pu_hbm, f_pu), (up_hbm, f_up), (uu_hbm, f_uu))]
    loads = [pltpu.make_async_copy(a, b, l_sem.at[i]) for i, (a, b) in enumerate(pairs)]
    for load in loads:
        load.start()

    barrier = pltpu.get_barrier_semaphore()

    def signal(dev):
        pl.semaphore_signal(barrier, inc=1, device_id=dev, device_id_type=MESH)

    for d in NEAR:
        signal(z_dev(d))
        signal(diagonal(d))
    signal(y_dev)
    signal(c_dev)
    for d in range(1, 4):
        signal((p, q_at(0, d)))
        signal((p, q_at(d, 0)))
    pl.when(moves)(lambda: signal((move_src, q)))

    def needed(a, qq):
        if a in (LP, PLO):
            return qq <= t
        if a in (PUP, UP):
            return qq >= t
        return None

    def when(cond, fn):
        if cond is None:
            fn()
        else:
            pl.when(cond)(fn)

    def f_copy(a, part, dev, i):
        block = factors[a].at[part, c]
        return pltpu.make_async_remote_copy(
            src_ref=block, dst_ref=block, send_sem=f_send.at[a], recv_sem=f_recv.at[a, i],
            device_id=dev, device_id_type=MESH,
        )

    def in_column(a, xx):
        return jnp.clip(t - 4 * xx + 1 if a in (LP, PLO) else 4 * xx + 4 - t, 0, 4)

    def d_copy(a, part):
        block = factors[a].at[part, c]
        return pltpu.make_async_remote_copy(
            src_ref=block, dst_ref=block, send_sem=d_send.at[a], recv_sem=d_recv.at[a],
            device_id=c_dev, device_id_type=MESH,
        )

    def send_x(a, qq):
        for dx in TURN:
            f_copy(a, qq, (p, q_at(dx, 0)), 3 + TURN.index(4 - dx)).start()

    def f_y(a):
        return [
            lambda dy=dy: when(needed(a, q), f_copy(a, q, (p, q_at(0, dy)), TURN.index(4 - dy)).start)
            for dy in TURN
        ]

    def f_x(a):
        def go():
            when(needed(a, q), lambda: send_x(a, q))
            d_copy(a, q).start()
        return [go]

    def f_turn(a):
        def step(dy):
            qq = q_at(0, dy)

            def go():
                f_copy(a, qq, c_dev, TURN.index(dy)).wait_recv()
                send_x(a, qq)
            when(needed(a, qq), go)
            d_copy(a, qq).start()
        return [lambda dy=dy: step(dy) for dy in TURN]

    def f_last(a):
        def step(dx):
            xx = lax.rem(x + dx, 4)

            def arrived(n):
                f_copy(a, pl.ds(4 * xx, n), c_dev, 3 + TURN.index(dx)).wait_recv()
            if needed(a, q) is None:
                arrived(4)
            else:
                for n in range(1, 5):
                    pl.when(in_column(a, xx) == n)(lambda n=n: arrived(n))
            d_copy(a, pl.ds(4 * xx, 4)).start()
        return [lambda dx=dx: step(dx) for dx in TURN]

    def f_ready(a):
        d_copy(a, pl.ds(0, NT)).wait_recv()

    def f_drain(a):
        def sent(n):
            part = factors[a].at[pl.ds(0, 3 * n), 0]
            pltpu.make_async_remote_copy(
                src_ref=part, dst_ref=part, send_sem=f_send.at[a], recv_sem=f_recv.at[a, 0],
                device_id=c_dev, device_id_type=MESH,
            ).wait_send()
        if needed(a, q) is None:
            sent(5)
        else:
            count = in_column(a, x) + jnp.where(needed(a, q), 1, 0)
            for n in range(1, 6):
                pl.when(count == n)(lambda n=n: sent(n))
        d_copy(a, pl.ds(0, NT)).wait_send()

    def run(*steps):
        for group in steps:
            for step in group:
                step()

    def g_copy(s, h, tt, dev, sem):
        block = v.at[s, h, tt]
        return pltpu.make_async_remote_copy(
            src_ref=block, dst_ref=block, send_sem=g_send.at[0], recv_sem=sem,
            device_id=dev, device_id_type=MESH,
        )

    def g_start(s, h):
        for d in NEAR:
            g_copy(s, h, t, z_dev(d), g_recv.at[SLOT[s], h, NEAR.index(NZ - d)]).start()
        g_copy(s, h, t, y_dev, y_recv.at[s, h]).start()

    def g_turn(s, h, steps=()):
        far = g_recv.at[SLOT[s], h, 4]
        for i, d in enumerate(NEAR):
            tt = yl * NZ + z_at(d)
            g_copy(s, h, tt, y_dev, g_recv.at[SLOT[s], h, i]).wait_recv()

            def relay(e):
                g_copy(s, h, tt, z_dev(e), far).start()
                g_copy(s, h, tt, diagonal(e), y_recv.at[s, h]).start()

            if d == 2:
                relay(7)
                pl.when(first_core)(lambda: relay(6))
            if d == 6:
                relay(1)
                pl.when(jnp.logical_not(first_core))(lambda: relay(2))
            g_copy(s, h, tt, y_dev, y_recv.at[s, h]).start()
            run(steps[len(steps) * i // 4 : len(steps) * (i + 1) // 4])

    def g_far(s, h):
        g_copy(s, h, pl.ds(0, 3), y_dev, g_recv.at[SLOT[s], h, 4]).wait_recv()

    def turns(s, *steps):
        for h in range(H):
            with jax.named_scope("near%d_%d" % (h, s)):
                g_turn(s, h, steps[h] if h < len(steps) else ())

    def fars(s):
        for h in range(H):
            with jax.named_scope("far%d_%d" % (h, s)):
                g_far(s, h)

    def g_last(s, h):
        g_copy(s, h, pl.ds((1 - yl) * NZ, NZ), y_dev, y_recv.at[s, h]).wait_recv()

    def g_drain():
        part = v.at[:, :, pl.ds(0, 15)]
        pltpu.make_async_remote_copy(
            src_ref=part, dst_ref=part, send_sem=g_send.at[0], recv_sem=y_recv.at[0, 0],
            device_id=y_dev, device_id_type=MESH,
        ).wait_send()

    def e_copy(i, src, dst):
        return pltpu.make_async_remote_copy(
            src_ref=src, dst_ref=dst, send_sem=e_send.at[i], recv_sem=e_recv.at[i],
            device_id=c_dev, device_id_type=MESH,
        )

    mine = pl.ds(pl.multiple_of(64 * c, 64), 64)
    other = pl.ds(pl.multiple_of(64 - 64 * c, 64), 64)
    x_ex = e_copy(0, x_out.at[other], x_in)
    u_ex = e_copy(1, u_out.at[other], u_in)
    par_ex = e_copy(2, par_out.at[other], par_in)
    sol_ex = e_copy(3, sol_out, sol_in)
    ch_ex = e_copy(4, ch_out, ch_in)


    def ordered(own, got):
        return jnp.where(first_core, own, got), jnp.where(first_core, got, own)

    low = lax.broadcasted_iota(jnp.int32, (64, 128), 1) < 64

    def swap_halves(a, b):
        return jnp.where(low, a, pltpu.roll(b, 64, 1)), jnp.where(low, pltpu.roll(a, 64, 1), b)

    with jax.named_scope("prep"):
        loads[1].wait()
        x_out[...] = jnp.concatenate([pivot_ref[0], pivot_ref[1]], axis=0).T.astype(BF).astype(F32)

        loads[0].wait()
    with jax.named_scope("barrier"):
        pl.semaphore_wait(barrier, 8 + 2 + 6 + jnp.where(moves, 1, 0))

    own_lu = f_lu.at[q, c]
    lu_move = pltpu.make_async_remote_copy(
        src_ref=lu_ref, dst_ref=f_lu.at[q, p // 16], send_sem=m_send.at[0], recv_sem=m_recv.at[0],
        device_id=(move_dst, q), device_id_type=MESH,
    )
    upd_move = pltpu.make_async_remote_copy(
        src_ref=update_ref, dst_ref=upd_in, send_sem=m_send.at[1], recv_sem=m_recv.at[1],
        device_id=(move_dst, q), device_id_type=MESH,
    )
    lu_arrival = pltpu.make_async_remote_copy(
        src_ref=own_lu, dst_ref=own_lu, send_sem=m_send.at[0], recv_sem=m_recv.at[0],
        device_id=c_dev, device_id_type=MESH,
    )
    x_ex.start()
    pl.when(moves)(lu_move.start)

    @pl.when(jnp.logical_not(moves))
    def _():
        f_lu[q, c] = lu_ref[...]

    with jax.named_scope("x_ex"):
        x_ex.wait_recv()
    x0, x1 = swap_halves(*ordered(x_out[mine, :], x_in[...]))
    xt = jnp.concatenate([x0, x1], axis=1).astype(BF)
    for h in range(H):
        v[X, h, t] = xt[W * h : W * (h + 1)]
        g_start(X, h)

    for load in loads[2:]:
        load.wait()
    run(f_x(PLO), f_x(LP), f_x(PUP))
    def clear(f, i):
        @pl.when(i != q)
        def _():
            f[i, c] = jnp.zeros(f.shape[2:], BF)

    def zero_fill(i, _):
        @pl.when(i > t)
        def _():
            clear(f_lp, i)
            clear(f_pl, i)

        @pl.when(i < t)
        def _():
            clear(f_up, i)
            clear(f_pu, i)

        return 0

    lax.fori_loop(0, NT, zero_fill, 0)
    pl.when(moves)(upd_move.start)

    @pl.when(jnp.logical_not(moves))
    def _():
        upd_in[...] = update_ref[...]

    par_out[...] = parent_ref[...].T
    par_ex.start()
    with jax.named_scope("w_lu_move"):
        pl.when(moves)(lu_arrival.wait_recv)
    run(f_y(LU), f_x(LU))
    turns(X, f_y(PLO), f_turn(LU))
    fars(X)
    with jax.named_scope("w_upd"):
        pl.when(moves)(upd_move.wait_recv)
        u_out[...] = upd_in[...].T
    u_ex.start()

    row = lax.broadcasted_iota(jnp.int32, (256, 128), 0)

    def selection(k):
        return jnp.where(row == maps_ref[pl.ds(16 * k + t, 1), :] - 256 * t, 1.0, 0.0).astype(BF)

    select = (selection(0), selection(1))

    def line(s, h, side):
        first = side * NZ
        return [v[s, h, first + j] for j in range(NZ)], [first + j for j in range(NZ)]

    def apply_parent(s, h, f, side):
        blocks, at = line(s, h, side)
        left = jnp.concatenate(blocks, axis=1)
        right = jnp.concatenate([f[i].reshape(256, 256) for i in at], axis=1)
        return dot(left, right)

    def apply_child(s, h, f, side):
        blocks, at = line(s, h, side)
        out = []
        for k in range(2):
            left = jnp.concatenate([b[:, 128 * k : 128 * (k + 1)] for b in blocks], axis=1)
            if f is f_lu:
                right = jnp.concatenate([f[i, k] for i in at], axis=1)
            else:
                right = jnp.concatenate(
                    [jnp.concatenate([f[i, 0, k], f[i, 1, k]], axis=0) for i in at], axis=1
                )
            out.append(dot(left, right))
        return jnp.concatenate(out, axis=1)

    def both(fn, s, h, f):
        return fn(s, h, f, yl) + fn(s, h, f, 1 - yl)

    run(f_y(LP))
    with jax.named_scope("lu_last"):
        run(f_last(LU)[:2], f_y(PUP), f_last(LU)[2:])
    with jax.named_scope("pl_turn"):
        run(f_turn(PLO))
    with jax.named_scope("x_last"):
        g_last(X, 0)
    with jax.named_scope("lu_ready"):
        f_ready(LU)
    with jax.named_scope("ex_upd_par"):
        par_ex.wait_recv()
        u_ex.wait_recv()
    upd = ordered(u_out[mine, :], u_in[...])
    par = jnp.concatenate(ordered(par_out[mine, :], par_in[...]), axis=1)
    for h in range(H):
        rows = slice(W * h, W * (h + 1))
        if h:
            with jax.named_scope("x_last1"):
                g_last(X, h)
        with jax.named_scope("mm_s"):
            u = both(apply_child, X, h, f_lu)
            u0 = (upd[0][rows] + u[:, :128]).astype(BF)
            u1 = (upd[1][rows] + u[:, 128:]).astype(BF)
            st = par[rows] + (dot(u0, select[0]) + dot(u1, select[1]))
            v[S, h, t] = st.astype(BF)
        g_start(S, h)

    def stage(src, f, a, steps, finish):
        turns(src, *steps[:2])
        with jax.named_scope("f_last_%d" % src):
            run(f_last(a))
        run(*steps[2:])
        fars(src)
        with jax.named_scope("f_ready_%d" % src):
            f_ready(a)
        with jax.named_scope("mm0_%d" % src):
            for h in range(H):
                acc_ref[h] = apply_parent(src, h, f, yl)
        for h in range(H):
            if h == 0:
                with jax.named_scope("hook_%d" % src):
                    run(f_turn(UU) + [pm_near] if src == M else f_last(LP))
            with jax.named_scope("last%d_%d" % (h, src)):
                g_last(src, h)
            with jax.named_scope("mm1_%d" % src):
                finish(h, acc_ref[h] + apply_parent(src, h, f, 1 - yl))

    def finish_m(h, acc):
        v[M, h, t] = acc.astype(BF)
        g_start(M, h)

    stage(S, f_pl, PLO, [f_turn(LP) + f_x(UP) + f_x(UU), f_turn(PUP), f_y(UP)], finish_m)

    sols = []

    def finish_r(h, acc):
        half = acc.astype(BF)
        r = [dot(half, select[k], CONTRACT_INNER) for k in range(2)]
        v[R, h, t] = jnp.concatenate(r, axis=1).astype(BF)
        g_start(R, h)
        sols.append(acc)

    def pm_start():
        for h in range(H):
            g_start(PM, h)

    def pm_near():
        with jax.named_scope("pm_near"):
            for h in range(H):
                g_turn(PM, h)

    run(f_y(UU))
    with jax.named_scope("lp_ready"):
        f_ready(LP)
    with jax.named_scope("mm_p"):
        for h in range(H):
            v[PM, h, t] = both(apply_child, X, h, f_lp).astype(BF)
    stage(M, f_pu, PUP, [[], f_turn(UP), [pm_start]], finish_r)

    sol = jnp.concatenate(sols, axis=0)
    own_sol, their_sol = ordered(sol[:, :128], sol[:, 128:])
    sol_out[...] = their_sol
    sol_ex.start()
    turns(R, f_last(UP), f_last(UU))
    fars(R)
    with jax.named_scope("pm_far"):
        for h in range(H):
            g_far(PM, h)
    with jax.named_scope("p_last"):
        for h in range(H):
            g_last(PM, h)
    with jax.named_scope("up_ready"):
        f_ready(UP)
        f_ready(UU)
    outs = []
    with jax.named_scope("mm_c0"):
        for h in range(H):
            acc_ref[h] = both(apply_child, PM, h, f_up) + apply_child(R, h, f_uu, yl)
    for h in range(H):
        with jax.named_scope("r_last%d" % h):
            g_last(R, h)
        with jax.named_scope("mm_c1"):
            outs.append(acc_ref[h] + apply_child(R, h, f_uu, 1 - yl))
    ch = jnp.concatenate(outs, axis=0)
    own_ch, their_ch = ordered(*swap_halves(ch[:, :128], ch[:, 128:]))
    ch_out[...] = their_ch
    ch_ex.start()
    with jax.named_scope("fin_sol"):
        sol_ex.wait_recv()
        sol_ref[...] = jnp.concatenate(ordered(own_sol, sol_in[...]), axis=0).T
    with jax.named_scope("drain"):
        g_drain()
        for a in range(6):
            f_drain(a)
        pl.when(moves)(lu_move.wait_send)
        pl.when(moves)(upd_move.wait_send)
        for e in (x_ex, u_ex, par_ex, sol_ex, ch_ex):
            e.wait_send()
    with jax.named_scope("fin_ch"):
        ch_ex.wait_recv()
        out = jnp.concatenate(ordered(own_ch, ch_in[...]), axis=0).T
        child_ref[0] = out[0:64]
        child_ref[1] = out[64:128]


def shards(pivot_rhs, update_rhs, parent_rhs, lower_pivot, lower_update, parent_lower, parent_upper, upper_pivot, upper_update, maps):
    vm = pl.BlockSpec(memory_space=pltpu.VMEM)
    dma = pltpu.SemaphoreType.DMA
    square = pltpu.VMEM((128, 128), F32)
    half = pltpu.VMEM((64, 128), F32)
    child_factor = pltpu.VMEM((NT, 2, 2, 64, 128), BF)
    parent_factor = pltpu.VMEM((NT, 2, 128, 256), BF)
    return pl.pallas_call(
        body,
        out_shape=(
            jax.ShapeDtypeStruct((128, 128), F32),
            jax.ShapeDtypeStruct((2, 64, 128), F32),
        ),
        in_specs=[pl.BlockSpec(memory_space=pltpu.HBM)] * 10,
        out_specs=(vm, vm),
        scratch_shapes=[
            pltpu.VMEM((5, H, NT, W, 256), BF),
            pltpu.VMEM((NT, 2, 128, 128), BF),
            child_factor,
            parent_factor,
            parent_factor,
            child_factor,
            child_factor,
            pltpu.VMEM((128, 128), BF),
            square,
            pltpu.VMEM((2, 64, 128), F32),
            square,
            pltpu.VMEM((32, 128), jnp.int32),
            square, square, half, square, half, square, half, half, half, half, half,
            pltpu.VMEM((H, W, 256), F32),
            dma((1,)),
            dma((3, H, 5)),
            dma((5, H)),
            dma((6,)),
            dma((6, 6)),
            dma((6,)),
            dma((6,)),
            dma((2,)),
            dma((2,)),
            dma((5,)),
            dma((5,)),
            dma((10,)),
        ],
        compiler_params=pltpu.CompilerParams(collective_id=0, has_side_effects=True, vmem_limit_bytes=60 << 20),
    )(
        pivot_rhs, update_rhs, parent_rhs, lower_pivot, lower_update, parent_lower, parent_upper,
        upper_pivot, upper_update, maps.reshape(32, 128),
    )


def solution(mesh):
    placed = (
        P(None, "panel", "rhs"),
        P("panel", "rhs"),
        P("panel", "rhs"),
        P(None, "panel", "rhs"),
        P("panel", "rhs"),
        P("panel", "rhs"),
        P("panel", "rhs"),
        P(None, "panel", "rhs"),
        P(None, "panel", "rhs"),
        P(),
    )
    return jax.shard_map(
        shards,
        mesh=mesh,
        in_specs=placed,
        out_specs=(P("panel", "rhs"), P(None, "panel", "rhs")),
        check_vma=False,
    )
```

```python
import jax
import jax.numpy as jnp
from jax import lax
from jax.experimental import pallas as pl
from jax.experimental.pallas import tpu as pltpu
from jax.sharding import PartitionSpec as P

MESH = pl.DeviceIdType.MESH
BF = jnp.bfloat16
F32 = jnp.float32
NZ = 8
NT = 16
H = 2
W = 64 // H
CONTRACT_LAST = (((1,), (1,)), ((), ()))
CONTRACT_INNER = (((1,), (0,)), ((), ()))
NEAR = (2, 6, 1, 7)
TURN = (1, 3, 2)

LU, LP, PLO, PUP, UP, UU = range(6)
X, S, M, R, PM = range(5)
SLOT = (0, 1, 0, 1, 2)


def dot(a, b, dims=CONTRACT_LAST):
    return lax.dot_general(a, b, dims, preferred_element_type=F32)


def body(
    pivot_hbm, update_hbm, parent_hbm, lp_hbm, lu_hbm, pl_hbm, pu_hbm, up_hbm, uu_hbm, maps_hbm,
    sol_ref, child_ref,
    v, f_lu, f_lp, f_pl, f_pu, f_up, f_uu,
    lu_ref, update_ref, pivot_ref, parent_ref, maps_ref,
    upd_in, x_out, x_in, u_out, u_in, par_out, par_in, sol_out, sol_in, ch_out, ch_in, acc_ref,
    g_send, g_recv, y_recv, f_send, f_recv, d_send, d_recv, m_send, m_recv, e_send, e_recv, l_sem,
):
    p = lax.axis_index("panel")
    q = lax.axis_index("rhs")
    c = lax.rem(p, 2)
    first_core = c == 0
    t = p // 2
    yl = t // NZ
    z = lax.rem(t, NZ)
    x = q // 4
    yh = lax.rem(q, 4)
    factors = (f_lu, f_lp, f_pl, f_pu, f_up, f_uu)

    def z_at(d):
        return lax.rem(z + d, NZ)

    def q_at(dx, dy):
        return lax.rem(x + dx, 4) * 4 + lax.rem(yh + dy, 4)

    def z_dev(d):
        return ((yl * NZ + z_at(d)) * 2 + c, q)

    def diagonal(d):
        return (((1 - yl) * NZ + z_at(d)) * 2 + c, q)

    y_dev = (((1 - yl) * NZ + z) * 2 + c, q)
    c_dev = (2 * t + 1 - c, q)
    move_src = 16 * c + t
    move_dst = 2 * lax.rem(p, 16) + p // 16
    moves = move_src != p

    pairs = [(lu_hbm, lu_ref), (pivot_hbm, pivot_ref), (update_hbm, update_ref), (parent_hbm, parent_ref), (maps_hbm, maps_ref)]
    pairs += [(h, f.at[q, c]) for h, f in ((lp_hbm, f_lp), (pl_hbm, f_pl), (pu_hbm, f_pu), (up_hbm, f_up), (uu_hbm, f_uu))]
    loads = [pltpu.make_async_copy(a, b, l_sem.at[i]) for i, (a, b) in enumerate(pairs)]
    for load in loads:
        load.start()

    barrier = pltpu.get_barrier_semaphore()

    def signal(dev):
        pl.semaphore_signal(barrier, inc=1, device_id=dev, device_id_type=MESH)

    for d in NEAR:
        signal(z_dev(d))
        signal(diagonal(d))
    signal(y_dev)
    signal(c_dev)
    for d in range(1, 4):
        signal((p, q_at(0, d)))
        signal((p, q_at(d, 0)))
    pl.when(moves)(lambda: signal((move_src, q)))

    def needed(a, qq):
        if a in (LP, PLO):
            return qq <= t
        if a in (PUP, UP):
            return qq >= t
        return None

    def when(cond, fn):
        if cond is None:
            fn()
        else:
            pl.when(cond)(fn)

    def f_copy(a, part, dev, i):
        block = factors[a].at[part, c]
        return pltpu.make_async_remote_copy(
            src_ref=block, dst_ref=block, send_sem=f_send.at[a], recv_sem=f_recv.at[a, i],
            device_id=dev, device_id_type=MESH,
        )

    def in_column(a, xx):
        return jnp.clip(t - 4 * xx + 1 if a in (LP, PLO) else 4 * xx + 4 - t, 0, 4)

    def d_copy(a, part):
        block = factors[a].at[part, c]
        return pltpu.make_async_remote_copy(
            src_ref=block, dst_ref=block, send_sem=d_send.at[a], recv_sem=d_recv.at[a],
            device_id=c_dev, device_id_type=MESH,
        )

    def send_x(a, qq):
        for dx in TURN:
            f_copy(a, qq, (p, q_at(dx, 0)), 3 + TURN.index(4 - dx)).start()

    def f_y(a):
        return [
            lambda dy=dy: when(needed(a, q), f_copy(a, q, (p, q_at(0, dy)), TURN.index(4 - dy)).start)
            for dy in TURN
        ]

    def f_x(a):
        def go():
            when(needed(a, q), lambda: send_x(a, q))
            d_copy(a, q).start()
        return [go]

    def f_turn(a):
        def step(dy):
            qq = q_at(0, dy)

            def go():
                f_copy(a, qq, c_dev, TURN.index(dy)).wait_recv()
                send_x(a, qq)
            when(needed(a, qq), go)
            d_copy(a, qq).start()
        return [lambda dy=dy: step(dy) for dy in TURN]

    def f_last(a):
        def step(dx):
            xx = lax.rem(x + dx, 4)

            def arrived(n):
                f_copy(a, pl.ds(4 * xx, n), c_dev, 3 + TURN.index(dx)).wait_recv()
            if needed(a, q) is None:
                arrived(4)
            else:
                for n in range(1, 5):
                    pl.when(in_column(a, xx) == n)(lambda n=n: arrived(n))
            d_copy(a, pl.ds(4 * xx, 4)).start()
        return [lambda dx=dx: step(dx) for dx in TURN]

    def f_ready(a):
        d_copy(a, pl.ds(0, NT)).wait_recv()

    def f_drain(a):
        def sent(n):
            part = factors[a].at[pl.ds(0, 3 * n), 0]
            pltpu.make_async_remote_copy(
                src_ref=part, dst_ref=part, send_sem=f_send.at[a], recv_sem=f_recv.at[a, 0],
                device_id=c_dev, device_id_type=MESH,
            ).wait_send()
        if needed(a, q) is None:
            sent(5)
        else:
            count = in_column(a, x) + jnp.where(needed(a, q), 1, 0)
            for n in range(1, 6):
                pl.when(count == n)(lambda n=n: sent(n))
        d_copy(a, pl.ds(0, NT)).wait_send()

    def run(*steps):
        for group in steps:
            for step in group:
                step()

    def g_copy(s, h, tt, dev, sem):
        block = v.at[s, h, tt]
        return pltpu.make_async_remote_copy(
            src_ref=block, dst_ref=block, send_sem=g_send.at[0], recv_sem=sem,
            device_id=dev, device_id_type=MESH,
        )

    def g_start(s, h):
        for d in NEAR:
            g_copy(s, h, t, z_dev(d), g_recv.at[SLOT[s], h, NEAR.index(NZ - d)]).start()
        g_copy(s, h, t, y_dev, y_recv.at[s, h]).start()

    def g_turn(s, h, steps=()):
        far = g_recv.at[SLOT[s], h, 4]
        for i, d in enumerate(NEAR):
            tt = yl * NZ + z_at(d)
            g_copy(s, h, tt, y_dev, g_recv.at[SLOT[s], h, i]).wait_recv()

            def relay(e):
                g_copy(s, h, tt, z_dev(e), far).start()
                g_copy(s, h, tt, diagonal(e), y_recv.at[s, h]).start()

            if d == 2:
                relay(7)
                pl.when(first_core)(lambda: relay(6))
            if d == 6:
                relay(1)
                pl.when(jnp.logical_not(first_core))(lambda: relay(2))
            g_copy(s, h, tt, y_dev, y_recv.at[s, h]).start()
            run(steps[len(steps) * i // 4 : len(steps) * (i + 1) // 4])

    def g_far(s, h):
        g_copy(s, h, pl.ds(0, 3), y_dev, g_recv.at[SLOT[s], h, 4]).wait_recv()

    def turns(s, *steps):
        for h in range(H):
            with jax.named_scope("near%d_%d" % (h, s)):
                g_turn(s, h, steps[h] if h < len(steps) else ())

    def fars(s):
        for h in range(H):
            with jax.named_scope("far%d_%d" % (h, s)):
                g_far(s, h)

    def g_last(s, h):
        g_copy(s, h, pl.ds((1 - yl) * NZ, NZ), y_dev, y_recv.at[s, h]).wait_recv()

    def g_drain():
        part = v.at[:, :, pl.ds(0, 15)]
        pltpu.make_async_remote_copy(
            src_ref=part, dst_ref=part, send_sem=g_send.at[0], recv_sem=y_recv.at[0, 0],
            device_id=y_dev, device_id_type=MESH,
        ).wait_send()

    def e_copy(i, src, dst):
        return pltpu.make_async_remote_copy(
            src_ref=src, dst_ref=dst, send_sem=e_send.at[i], recv_sem=e_recv.at[i],
            device_id=c_dev, device_id_type=MESH,
        )

    mine = pl.ds(pl.multiple_of(64 * c, 64), 64)
    other = pl.ds(pl.multiple_of(64 - 64 * c, 64), 64)
    x_ex = e_copy(0, x_out.at[other], x_in)
    u_ex = e_copy(1, u_out.at[other], u_in)
    par_ex = e_copy(2, par_out.at[other], par_in)
    sol_ex = e_copy(3, sol_out, sol_in)
    ch_ex = e_copy(4, ch_out, ch_in)


    def ordered(own, got):
        return jnp.where(first_core, own, got), jnp.where(first_core, got, own)

    low = lax.broadcasted_iota(jnp.int32, (64, 128), 1) < 64

    def swap_halves(a, b):
        return jnp.where(low, a, pltpu.roll(b, 64, 1)), jnp.where(low, pltpu.roll(a, 64, 1), b)

    with jax.named_scope("prep"):
        loads[1].wait()
        x_out[...] = jnp.concatenate([pivot_ref[0], pivot_ref[1]], axis=0).T.astype(BF).astype(F32)

        loads[0].wait()
    with jax.named_scope("barrier"):
        pl.semaphore_wait(barrier, 8 + 2 + 6 + jnp.where(moves, 1, 0))

    own_lu = f_lu.at[q, c]
    lu_move = pltpu.make_async_remote_copy(
        src_ref=lu_ref, dst_ref=f_lu.at[q, p // 16], send_sem=m_send.at[0], recv_sem=m_recv.at[0],
        device_id=(move_dst, q), device_id_type=MESH,
    )
    upd_move = pltpu.make_async_remote_copy(
        src_ref=update_ref, dst_ref=upd_in, send_sem=m_send.at[1], recv_sem=m_recv.at[1],
        device_id=(move_dst, q), device_id_type=MESH,
    )
    lu_arrival = pltpu.make_async_remote_copy(
        src_ref=own_lu, dst_ref=own_lu, send_sem=m_send.at[0], recv_sem=m_recv.at[0],
        device_id=c_dev, device_id_type=MESH,
    )
    x_ex.start()
    pl.when(moves)(lu_move.start)

    @pl.when(jnp.logical_not(moves))
    def _():
        f_lu[q, c] = lu_ref[...]

    with jax.named_scope("x_ex"):
        x_ex.wait_recv()
    x0, x1 = swap_halves(*ordered(x_out[mine, :], x_in[...]))
    xt = jnp.concatenate([x0, x1], axis=1).astype(BF)
    for h in range(H):
        v[X, h, t] = xt[W * h : W * (h + 1)]
        g_start(X, h)

    for load in loads[2:]:
        load.wait()
    run(f_x(PLO), f_x(LP), f_x(PUP))
    def clear(f, i):
        @pl.when(i != q)
        def _():
            f[i, c] = jnp.zeros(f.shape[2:], BF)

    def zero_fill(i, _):
        @pl.when(i > t)
        def _():
            clear(f_lp, i)
            clear(f_pl, i)

        @pl.when(i < t)
        def _():
            clear(f_up, i)
            clear(f_pu, i)

        return 0

    lax.fori_loop(0, NT, zero_fill, 0)
    pl.when(moves)(upd_move.start)

    @pl.when(jnp.logical_not(moves))
    def _():
        upd_in[...] = update_ref[...]

    par_out[...] = parent_ref[...].T
    par_ex.start()
    with jax.named_scope("w_lu_move"):
        pl.when(moves)(lu_arrival.wait_recv)
    run(f_y(LU), f_x(LU))
    turns(X, f_y(PLO), f_turn(LU))
    run(f_y(LP), f_y(PUP))
    fars(X)
    with jax.named_scope("w_upd"):
        pl.when(moves)(upd_move.wait_recv)
        u_out[...] = upd_in[...].T
    u_ex.start()

    row = lax.broadcasted_iota(jnp.int32, (256, 128), 0)

    def selection(k):
        return jnp.where(row == maps_ref[pl.ds(16 * k + t, 1), :] - 256 * t, 1.0, 0.0).astype(BF)

    select = (selection(0), selection(1))

    def line(s, h, side):
        first = side * NZ
        return [v[s, h, first + j] for j in range(NZ)], [first + j for j in range(NZ)]

    def apply_parent(s, h, f, side):
        blocks, at = line(s, h, side)
        left = jnp.concatenate(blocks, axis=1)
        right = jnp.concatenate([f[i].reshape(256, 256) for i in at], axis=1)
        return dot(left, right)

    def apply_child(s, h, f, side):
        blocks, at = line(s, h, side)
        out = []
        for k in range(2):
            left = jnp.concatenate([b[:, 128 * k : 128 * (k + 1)] for b in blocks], axis=1)
            if f is f_lu:
                right = jnp.concatenate([f[i, k] for i in at], axis=1)
            else:
                right = jnp.concatenate(
                    [jnp.concatenate([f[i, 0, k], f[i, 1, k]], axis=0) for i in at], axis=1
                )
            out.append(dot(left, right))
        return jnp.concatenate(out, axis=1)

    def both(fn, s, h, f):
        return fn(s, h, f, yl) + fn(s, h, f, 1 - yl)

    with jax.named_scope("lu_last"):
        run(f_last(LU))
    with jax.named_scope("pl_turn"):
        run(f_turn(PLO))
    with jax.named_scope("x_last"):
        g_last(X, 0)
    with jax.named_scope("lu_ready"):
        f_ready(LU)
    with jax.named_scope("ex_upd_par"):
        par_ex.wait_recv()
        u_ex.wait_recv()
    upd = ordered(u_out[mine, :], u_in[...])
    par = jnp.concatenate(ordered(par_out[mine, :], par_in[...]), axis=1)
    for h in range(H):
        rows = slice(W * h, W * (h + 1))
        if h:
            with jax.named_scope("x_last1"):
                g_last(X, h)
        with jax.named_scope("mm_s"):
            u = both(apply_child, X, h, f_lu)
            u0 = (upd[0][rows] + u[:, :128]).astype(BF)
            u1 = (upd[1][rows] + u[:, 128:]).astype(BF)
            st = par[rows] + (dot(u0, select[0]) + dot(u1, select[1]))
            v[S, h, t] = st.astype(BF)
        g_start(S, h)

    def stage(src, f, a, steps, finish):
        turns(src, *steps[:2])
        with jax.named_scope("f_last_%d" % src):
            run(f_last(a))
        run(*steps[2:])
        fars(src)
        with jax.named_scope("f_ready_%d" % src):
            f_ready(a)
        with jax.named_scope("mm0_%d" % src):
            for h in range(H):
                acc_ref[h] = apply_parent(src, h, f, yl)
        for h in range(H):
            if h == 0:
                with jax.named_scope("hook_%d" % src):
                    run([pm_near] if src == M else f_last(LP))
            with jax.named_scope("last%d_%d" % (h, src)):
                g_last(src, h)
            with jax.named_scope("mm1_%d" % src):
                finish(h, acc_ref[h] + apply_parent(src, h, f, 1 - yl))

    def finish_m(h, acc):
        v[M, h, t] = acc.astype(BF)
        g_start(M, h)

    run(f_y(UP))
    stage(S, f_pl, PLO, [f_turn(LP) + f_x(UP) + f_x(UU), f_turn(PUP), f_y(UU)], finish_m)

    sols = []

    def finish_r(h, acc):
        half = acc.astype(BF)
        r = [dot(half, select[k], CONTRACT_INNER) for k in range(2)]
        v[R, h, t] = jnp.concatenate(r, axis=1).astype(BF)
        g_start(R, h)
        sols.append(acc)

    def pm_start():
        for h in range(H):
            g_start(PM, h)

    def pm_near():
        with jax.named_scope("pm_near"):
            for h in range(H):
                g_turn(PM, h)

    with jax.named_scope("lp_ready"):
        f_ready(LP)
    with jax.named_scope("mm_p"):
        for h in range(H):
            v[PM, h, t] = both(apply_child, X, h, f_lp).astype(BF)
    stage(M, f_pu, PUP, [f_turn(UP), f_turn(UU), [pm_start]], finish_r)

    sol = jnp.concatenate(sols, axis=0)
    own_sol, their_sol = ordered(sol[:, :128], sol[:, 128:])
    sol_out[...] = their_sol
    sol_ex.start()
    turns(R, f_last(UP), f_last(UU))
    fars(R)
    with jax.named_scope("pm_far"):
        for h in range(H):
            g_far(PM, h)
    with jax.named_scope("p_last"):
        for h in range(H):
            g_last(PM, h)
    with jax.named_scope("up_ready"):
        f_ready(UP)
        f_ready(UU)
    outs = []
    with jax.named_scope("mm_c0"):
        for h in range(H):
            acc_ref[h] = both(apply_child, PM, h, f_up) + apply_child(R, h, f_uu, yl)
    for h in range(H):
        with jax.named_scope("r_last%d" % h):
            g_last(R, h)
        with jax.named_scope("mm_c1"):
            outs.append(acc_ref[h] + apply_child(R, h, f_uu, 1 - yl))
    ch = jnp.concatenate(outs, axis=0)
    own_ch, their_ch = ordered(*swap_halves(ch[:, :128], ch[:, 128:]))
    ch_out[...] = their_ch
    ch_ex.start()
    with jax.named_scope("fin_sol"):
        sol_ex.wait_recv()
        sol_ref[...] = jnp.concatenate(ordered(own_sol, sol_in[...]), axis=0).T
    with jax.named_scope("drain"):
        g_drain()
        for a in range(6):
            f_drain(a)
        pl.when(moves)(lu_move.wait_send)
        pl.when(moves)(upd_move.wait_send)
        for e in (x_ex, u_ex, par_ex, sol_ex, ch_ex):
            e.wait_send()
    with jax.named_scope("fin_ch"):
        ch_ex.wait_recv()
        out = jnp.concatenate(ordered(own_ch, ch_in[...]), axis=0).T
        child_ref[0] = out[0:64]
        child_ref[1] = out[64:128]


def shards(pivot_rhs, update_rhs, parent_rhs, lower_pivot, lower_update, parent_lower, parent_upper, upper_pivot, upper_update, maps):
    vm = pl.BlockSpec(memory_space=pltpu.VMEM)
    dma = pltpu.SemaphoreType.DMA
    square = pltpu.VMEM((128, 128), F32)
    half = pltpu.VMEM((64, 128), F32)
    child_factor = pltpu.VMEM((NT, 2, 2, 64, 128), BF)
    parent_factor = pltpu.VMEM((NT, 2, 128, 256), BF)
    return pl.pallas_call(
        body,
        out_shape=(
            jax.ShapeDtypeStruct((128, 128), F32),
            jax.ShapeDtypeStruct((2, 64, 128), F32),
        ),
        in_specs=[pl.BlockSpec(memory_space=pltpu.HBM)] * 10,
        out_specs=(vm, vm),
        scratch_shapes=[
            pltpu.VMEM((5, H, NT, W, 256), BF),
            pltpu.VMEM((NT, 2, 128, 128), BF),
            child_factor,
            parent_factor,
            parent_factor,
            child_factor,
            child_factor,
            pltpu.VMEM((128, 128), BF),
            square,
            pltpu.VMEM((2, 64, 128), F32),
            square,
            pltpu.VMEM((32, 128), jnp.int32),
            square, square, half, square, half, square, half, half, half, half, half,
            pltpu.VMEM((H, W, 256), F32),
            dma((1,)),
            dma((3, H, 5)),
            dma((5, H)),
            dma((6,)),
            dma((6, 6)),
            dma((6,)),
            dma((6,)),
            dma((2,)),
            dma((2,)),
            dma((5,)),
            dma((5,)),
            dma((10,)),
        ],
        compiler_params=pltpu.CompilerParams(collective_id=0, has_side_effects=True, vmem_limit_bytes=60 << 20),
    )(
        pivot_rhs, update_rhs, parent_rhs, lower_pivot, lower_update, parent_lower, parent_upper,
        upper_pivot, upper_update, maps.reshape(32, 128),
    )


def solution(mesh):
    placed = (
        P(None, "panel", "rhs"),
        P("panel", "rhs"),
        P("panel", "rhs"),
        P(None, "panel", "rhs"),
        P("panel", "rhs"),
        P("panel", "rhs"),
        P("panel", "rhs"),
        P(None, "panel", "rhs"),
        P(None, "panel", "rhs"),
        P(),
    )
    return jax.shard_map(
        shards,
        mesh=mesh,
        in_specs=placed,
        out_specs=(P("panel", "rhs"), P(None, "panel", "rhs")),
        check_vma=False,
    )
```
